256 devices in a mesh: layer: 2 (over x_lo), row: 8 (over z), col: 16 (over y, x_hi, core).
Axes of the slice: x: 4 (x_hi: 2, x_lo: 2; x = x_hi * 2 + x_lo), y: 4, z: 8, core: 2. Of those that a mesh axis runs over, the one named last changes fastest.
Arguments:
- left_matrix: float32 [2, 2048, 16384], P(None, 'row', 'col'), may hold values from -6 to 6
- right_matrix: float32 [2, 16384, 2048], P(None, 'row', 'col'), may hold values from -0.03125 to 0.03125
Outputs:
- product: float32 [2, 2048, 2048], P(None, 'row', 'col')
The draws below stay inside these ranges and needn't reach their ends.
All inputs are finite; a program needn't handle non-finite values.
Results may differ from the reference program's by a relative error of at most 0.000071.
Values sent between devices are 32-bit elements; how exact they have to be, the bound alone decides.
A program may use at most 128 MiB of HBM per device.

```python
import jax
import jax.numpy as jnp
from jax import lax

K = 16384
M = 2048
NC = 2048


def block_scale(key, dims, cuts, smallest, largest):
    gain, own = 1.0, jax.random.fold_in(key, 6)
    for axis_at, shards_of in cuts:
        draws = jnp.exp(jax.random.uniform(jax.random.fold_in(own, axis_at), (shards_of,), jnp.float32, smallest / len(cuts), largest / len(cuts)))
        gain = gain * jnp.repeat(draws, dims[axis_at] // shards_of).reshape([-1 if axis == axis_at else 1 for axis in range(len(dims))])
    return gain


def gaussian(own_key, dims, width, most, cuts=(), kind=jnp.bfloat16):
    entries = width * jax.random.normal(own_key, dims, jnp.float32)
    if cuts:
        entries = entries * block_scale(own_key, dims, cuts, -0.22, 0.18)
    return jnp.clip(entries, -most, most).astype(kind)


def setup_inputs(seed: int = 0) -> dict:
    splits = jax.random.split(jax.random.key(seed), 3)
    left_matrix = gaussian(splits[0], (2, M, K), 1.0, 6.0, ((1, 8), (2, 16)), jnp.float32)
    right_matrix = gaussian(splits[1], (2, K, NC), (2 * K) ** -0.5, 0.03125, ((1, 8), (2, 16)), jnp.float32)
    return dict(left_matrix=left_matrix, right_matrix=right_matrix)


def reference(left_matrix, right_matrix):
    highest = lax.Precision.HIGHEST
    left_real = left_matrix[0]
    left_imag = left_matrix[1]
    right_real = right_matrix[0]
    right_imag = right_matrix[1]
    first_term = jnp.dot(left_real, right_real, precision=highest, preferred_element_type=jnp.float32)
    second_term = jnp.dot(left_imag, right_imag, precision=highest, preferred_element_type=jnp.float32)
    third_term = jnp.dot(left_real + left_imag, right_real + right_imag, precision=highest, preferred_element_type=jnp.float32)
    return jnp.stack([first_term - second_term, third_term - first_term - second_term])
```

```python
import jax
import jax.numpy as jnp
from jax import lax
from jax.sharding import PartitionSpec as P


def total_of_pieces(array, axis):
    return lax.all_gather(array, axis).sum(0)


def gauss_fold(right_whole, site_rows, cols_out):
    right_real = right_whole[0]
    right_imag = right_whole[1]
    right_total = right_real + right_imag
    highest = lax.Precision.HIGH
    empty = jnp.zeros((site_rows, cols_out), jnp.float32)

    def accumulate(totals, segment, offset):
        left_real = segment[0]
        left_imag = segment[1]
        first_term = jnp.dot(
            left_real, right_real, precision=highest, preferred_element_type=jnp.float32
        )
        second_term = jnp.dot(
            left_imag, right_imag, precision=highest, preferred_element_type=jnp.float32
        )
        third_term = jnp.dot(
            left_real + left_imag,
            right_total,
            precision=highest,
            preferred_element_type=jnp.float32,
        )
        return (first_term, second_term, third_term)

    return (accumulate, (empty, empty, empty))


def combine_terms(totals):
    first_term, second_term, third_term = totals
    return jnp.stack([first_term - second_term, third_term - first_term - second_term])


def local(left_matrix, right_matrix):
    layers = lax.axis_size("layer")
    layer_index = lax.axis_index("layer")
    local_rows = left_matrix.shape[1]
    local_cols = right_matrix.shape[2]
    left_width = left_matrix.shape[2]
    right_height = right_matrix.shape[1]
    share_width = left_width // layers
    group_count = right_height // left_width
    left_own = lax.dynamic_slice_in_dim(left_matrix, layer_index * share_width, share_width, 2)
    right_view = right_matrix.reshape(2, group_count, layers, share_width, local_cols)
    right_own = lax.dynamic_slice_in_dim(right_view, layer_index, 1, 2)
    right_own = right_own.reshape(2, group_count * share_width, local_cols)
    right_whole = lax.all_gather(right_own, "row", axis=1, tiled=True)
    accumulate, initial = gauss_fold(right_whole, local_rows, local_cols)
    totals = accumulate(initial, lax.all_gather(left_own, "col", axis=2, tiled=True), jnp.int32(0))
    partial_product = combine_terms(totals)
    product = total_of_pieces(partial_product, "layer")
    return product


def solution(mesh):
    in_specs = (P(None, "row", "col"), P(None, "row", "col"))
    out_specs = P(None, "row", "col")
    return jax.shard_map(local, mesh=mesh, in_specs=in_specs, out_specs=out_specs, check_vma=False)
```

```python
import functools

import jax
import jax.numpy as jnp
from jax import lax
from jax.experimental import pallas as pl
from jax.experimental.pallas import tpu as pltpu
from jax.sharding import PartitionSpec as P

MESH = pl.DeviceIdType.MESH
GROUPS = 4
NEAR_FIRST = (0, 1, 7, 2, 6, 3, 5, 4)
FAR_FIRST = (4, 3, 5, 2, 6, 1, 7)
CHUNKS = 4


def bulk_wait(ref, sem):
    pltpu.make_async_copy(ref, ref, sem).wait()


def kernel(
    left_ref, right_ref, out_ref,
    s1, ag, braw, bs, asp, cp, cr, fin, outs,
    a1_send, a1_recv, a2_send, ag_recv, a3_send,
    b_send, b_own, b_par, b_oth, b_oc,
    c_send, c_recv, x_send, x_recv,
):
    G = GROUPS
    l = lax.axis_index("layer")
    z = lax.axis_index("row")
    q = lax.axis_index("col")
    c = q % 2
    h = (q // 2) % 2
    y = q // 4
    a = 2 * h + l
    rg = s1.shape[3]
    width = s1.shape[4]
    sub_rows = rg * G
    mine = a * 2 + c
    slot = h * 2 + c

    def col_of(yy, hh, cc):
        return yy * 4 + hh * 2 + cc

    def dev(dl=0, dz=0, dy=0, dh=0, dc=0):
        return ((l + dl) % 2, (z + dz) % 8, col_of((y + dy) % 4, (h + dh) % 2, (c + dc) % 2))

    def send(src, dst, send_sem, recv_sem, device):
        pltpu.make_async_remote_copy(
            src_ref=src, dst_ref=dst, send_sem=send_sem, recv_sem=recv_sem,
            device_id=device, device_id_type=MESH,
        ).start()

    partners = set()
    for dx in (0, 1):
        for dy in range(4):
            for dc in range(2):
                partners.add((dx, 0, dy, dx, dc))
    for dz in range(1, 8):
        partners.add((0, dz, 0, 0, 0))
    for dl in range(2):
        for dh in range(2):
            for dc in range(2):
                partners.add((dl, 0, 0, dh, dc))
    partners.discard((0, 0, 0, 0, 0))
    partners = sorted(partners)
    barrier = pltpu.get_barrier_semaphore()
    for partner in partners:
        pl.semaphore_signal(barrier, inc=1, device_id=dev(*partner), device_id_type=MESH)
    pl.semaphore_wait(barrier, len(partners))

    def scatter(g):
        for dx in (1, 0):
            at = (2 * h + l) if dx == 0 else (2 * (1 - h) + (1 - l))
            for dy in (2, 1, 3, 0):
                for dc in (1, 0):
                    rows = (at * 2 + (c + dc) % 2) * sub_rows + g * rg
                    src = left_ref.at[
                        :,
                        pl.ds(pl.multiple_of(rows, rg), rg),
                        pl.ds(pl.multiple_of(((y + dy) % 4) * width, width), width),
                    ]
                    dst = s1.at[g, q]
                    if (dx, dy, dc) == (0, 0, 0):
                        pltpu.make_async_copy(src, dst, a1_recv.at[g, q // 2]).start()
                    else:
                        send(src, dst, a1_send.at[g], a1_recv.at[g, q // 2], dev(dx, 0, dy, dx, dc))

    def to_planes(g):
        for dz in FAR_FIRST:
            k = (z + dz) % 8
            piece = s1.at[g, pl.ds(2 * k, 2)]
            bulk_wait(piece, a1_recv.at[g, k])
            send(piece, ag.at[g, y, :, :, z], a2_send.at[g], ag_recv.at[g, y, z], dev(0, dz))
        bulk_wait(s1.at[g, pl.ds(2 * z, 2)], a1_recv.at[g, z])
        ag[g, y, :, :, z] = s1[g, pl.ds(2 * z, 2)]

    def along_y(g):
        for dz in NEAR_FIRST:
            r = (z + dz) % 8
            piece = ag.at[g, y, :, :, r]
            if dz:
                bulk_wait(piece, ag_recv.at[g, y, r])
                src = piece
            else:
                src = s1.at[g, pl.ds(2 * z, 2)]
            for dy in (1, 3):
                send(src, piece, a3_send.at[g], ag_recv.at[g, y, r], dev(0, 0, dy))

    def relay(g):
        for i, dz in enumerate(NEAR_FIRST):
            r = (z + dz) % 8
            back, onward = (3, 1) if i % 2 == 0 else (1, 3)
            origin = (y + back) % 4
            piece = ag.at[g, origin, :, :, r]
            bulk_wait(piece, ag_recv.at[g, origin, r])
            send(piece, piece, a3_send.at[g], ag_recv.at[g, origin, r], dev(0, 0, onward))

    def settle(g):
        for i, dz in enumerate(NEAR_FIRST):
            r = (z + dz) % 8
            for dy in (1 if i % 2 == 0 else 3, 2):
                origin = (y + dy) % 4
                bulk_wait(ag.at[g, origin, :, :, r], ag_recv.at[g, origin, r])

    depth = braw.shape[2]
    half = depth // 2
    chunk = half // CHUNKS
    other = (1 - h) * 2 + c
    cross = (1 - h) * 2 + (1 - c)

    def piece_rows(which, i):
        return pl.ds(pl.multiple_of(which * half + i * chunk, chunk), chunk)

    def right_out():
        pltpu.make_async_copy(right_ref, braw.at[slot], b_own).start()
        send(right_ref, braw.at[slot], b_send, b_par, dev(dc=1))
        for i in range(CHUNKS):
            rows = piece_rows(1 - l, i)
            send(right_ref.at[:, rows], braw.at[slot, :, rows], b_send, b_oth.at[1 - l, i], dev(1, 0, 0, 1, 0))

    def right_on():
        for i in range(CHUNKS):
            rows = piece_rows(l, i)
            piece = braw.at[other, :, rows]
            bulk_wait(piece, b_oth.at[l, i])
            send(piece, piece, b_send, b_oth.at[l, i], dev(dl=1))
            send(piece, piece, b_send, b_oc.at[l, i], dev(dc=1))

    def right_over():
        for i in range(CHUNKS):
            rows = piece_rows(1 - l, i)
            piece = braw.at[other, :, rows]
            bulk_wait(piece, b_oth.at[1 - l, i])
            send(piece, piece, b_send, b_oc.at[1 - l, i], dev(dc=1))

    def split(x):
        high = x.astype(jnp.bfloat16)
        return high, (x - high.astype(jnp.float32)).astype(jnp.bfloat16)

    def split_right(which, rows):
        cols = pl.ds(pl.multiple_of(which * 128, 128), 128)
        real = braw[which, 0, rows, :]
        imag = braw[which, 1, rows, :]
        for m, x in enumerate((real, imag, real + imag)):
            high, low = split(x)
            bs[m, 0, rows, cols] = high
            bs[m, 1, rows, cols] = low

    def split_whole(which):
        @pl.loop(0, depth // 128)
        def _(i):
            split_right(which, pl.ds(pl.multiple_of(i * 128, 128), 128))

    lines = 8 * rg

    def multiply(g):
        for t in range(8):
            for_k, from_y = t // 4, t % 4
            real = ag[g, from_y, for_k, 0].reshape(lines, width)
            imag = ag[g, from_y, for_k, 1].reshape(lines, width)
            for m, x in enumerate((real, imag, real + imag)):
                high, low = split(x)
                asp[m, :lines, t * width:(t + 1) * width] = high
                asp[m, lines:, t * width:(t + 1) * width] = low
        terms = []
        for m in range(3):
            both = jnp.dot(asp[m], bs[m, 0], preferred_element_type=jnp.float32)
            rest = jnp.dot(asp[m, :lines], bs[m, 1], preferred_element_type=jnp.float32)
            terms.append(both[:lines] + both[lines:] + rest)
        first, second, third = terms
        cp[g, :, 0] = (first - second).reshape(8, rg, 512)
        cp[g, :, 1] = (third - first - second).reshape(8, rg, 512)

    def hand_back(g):
        for dz in FAR_FIRST:
            r = (z + dz) % 8
            send(cp.at[g, r], cr.at[g, z], c_send.at[g], c_recv.at[g, z], dev(0, dz))

    def add_up(g):
        total = cp[g, z]
        for dz in NEAR_FIRST[1:]:
            k = (z + dz) % 8
            bulk_wait(cr.at[g, k], c_recv.at[g, k])
            total = total + cr[g, k]
        for i in range(4):
            fin[g, i] = total[:, :, i * 128:(i + 1) * 128]
        for dl in (1, 0):
            for dh in (1, 0):
                for dc in (1, 0):
                    target = ((h + dh) % 2) * 2 + (c + dc) % 2
                    if dl or dh or dc:
                        send(fin.at[g, target], outs.at[g, mine], x_send.at[g], x_recv.at[g], dev(dl, 0, 0, dh, dc))
        outs[g, mine] = fin[g, slot]

    def finish(g):
        bulk_wait(outs.at[g, pl.ds(0, 7)], x_recv.at[g])
        for i in range(8):
            out_ref[:, i * sub_rows + g * rg:i * sub_rows + (g + 1) * rg, :] = outs[g, i]

    for g in range(G):
        scatter(g)
    right_out()
    to_planes(0)
    to_planes(1)
    along_y(0)
    to_planes(2)
    along_y(1)
    relay(0)
    to_planes(3)
    along_y(2)
    relay(1)
    bulk_wait(braw.at[slot], b_own)
    split_whole(slot)
    bulk_wait(braw.at[h * 2 + 1 - c], b_par)
    split_whole(h * 2 + 1 - c)
    right_on()
    along_y(3)
    relay(2)
    right_over()
    split_whole(other)
    for i in range(CHUNKS):
        for which in (l, 1 - l):
            bulk_wait(braw.at[cross, :, piece_rows(which, i)], b_oc.at[which, i])
    split_whole(cross)
    settle(0)
    multiply(0)
    hand_back(0)
    settle(1)
    relay(3)
    multiply(1)
    hand_back(1)
    add_up(0)
    settle(2)
    multiply(2)
    hand_back(2)
    add_up(1)
    settle(3)
    multiply(3)
    hand_back(3)
    add_up(2)
    add_up(3)
    for g in range(G):
        finish(g)
    for g in range(G):
        bulk_wait(s1.at[g, pl.ds(0, 15)], a1_send.at[g])
        bulk_wait(s1.at[g, pl.ds(0, 14)], a2_send.at[g])
        bulk_wait(ag.at[g, pl.ds(0, 3)], a3_send.at[g])
        bulk_wait(cr.at[g, pl.ds(0, 7)], c_send.at[g])
        bulk_wait(outs.at[g, pl.ds(0, 7)], x_send.at[g])
    bulk_wait(braw.at[pl.ds(0, 3)], b_send)


def local(left_matrix, right_matrix):
    _, rows, left_width = left_matrix.shape
    _, depth, cols = right_matrix.shape
    G = GROUPS
    rg = rows // 8 // G
    width = left_width // 4
    f32, bf16 = jnp.float32, jnp.bfloat16
    dma = pltpu.SemaphoreType.DMA
    return pl.pallas_call(
        kernel,
        out_shape=jax.ShapeDtypeStruct((2, rows, cols), f32),
        in_specs=[pl.BlockSpec(memory_space=pl.ANY)] * 2,
        out_specs=pl.BlockSpec(memory_space=pltpu.VMEM),
        scratch_shapes=[
            pltpu.VMEM((G, 16, 2, rg, width), f32),
            pltpu.VMEM((G, 4, 2, 2, 8, rg, width), f32),
            pltpu.VMEM((4, 2, depth, cols), f32),
            pltpu.VMEM((3, 2, depth, 4 * cols), bf16),
            pltpu.VMEM((3, 16 * rg, depth), bf16),
            pltpu.VMEM((G, 8, 2, rg, 4 * cols), f32),
            pltpu.VMEM((G, 8, 2, rg, 4 * cols), f32),
            pltpu.VMEM((G, 4, 2, rg, cols), f32),
            pltpu.VMEM((G, 8, 2, rg, cols), f32),
            dma((G,)), dma((G, 8)), dma((G,)), dma((G, 4, 8)), dma((G,)),
            dma, dma, dma, dma((2, CHUNKS)), dma((2, CHUNKS)),
            dma((G,)), dma((G, 8)), dma((G,)), dma((G,)),
        ],
        compiler_params=pltpu.CompilerParams(
            collective_id=0, has_side_effects=True, vmem_limit_bytes=60 * 1024 * 1024
        ),
    )(left_matrix, right_matrix)


def solution(mesh):
    spec = P(None, "row", "col")
    return jax.shard_map(local, mesh=mesh, in_specs=(spec, spec), out_specs=spec, check_vma=False)
```

```python
import functools

import jax
import jax.numpy as jnp
from jax import lax
from jax.experimental import pallas as pl
from jax.experimental.pallas import tpu as pltpu
from jax.sharding import PartitionSpec as P

MESH = pl.DeviceIdType.MESH
GROUPS = 4
FAR_FIRST = (4, 3, 5, 2, 6, 1, 7)
ARRIVAL = (0, *FAR_FIRST)
ARRIVED = ((0,), (1,), (2, 3), (4, 5), (6, 7))
RELAYED = ((0, 2), (1, 3), (4, 6), (5, 7))
RELAY_OF = {i: j for j, pair in enumerate(RELAYED) for i in pair}
CHUNKS = 16


SCATTER, NEAR, FAR, PARTNER, PLANES, Y, RELAY, ON, OVER, CROSS, SETTLE, SPLIT, MUL, BACK, ADD, FINISH, DRAIN = range(17)
PARTS = (((0, 2), (2, 3), (3, 4)), ((0, 2), (2, 3), (3, 4)), ((0, 2), (2, 4)), ((0, 2), (2, 4)))
ORDER = (
    (SCATTER, 0), (NEAR,), (SCATTER, 1), (SCATTER, 2), (PARTNER,), (FAR, 0), (PLANES, 0), (Y, 0, 0, 1),
    (FAR, 1), (FAR, 2), (PLANES, 1), (Y, 1, 0, 1), (FAR, 3), (FAR, 4), (Y, 0, 1, 2), (PLANES, 2),
    (Y, 2, 0, 1), (FAR, 5), (Y, 0, 2, 3), (ON, 0), (Y, 0, 3, 4), (FAR, 6), (ON, 1), (Y, 0, 4, 5),
    (FAR, 7), (ON, 2), (RELAY, 0, 0, 1), (OVER, 0), (RELAY, 0, 1, 2), (FAR, 8), (ON, 3), (Y, 1, 1, 2),
    (OVER, 1), (FAR, 9), (Y, 1, 2, 3), (ON, 4), (RELAY, 0, 2, 3), (OVER, 2), (Y, 1, 3, 4),
    (RELAY, 0, 3, 4), (FAR, 10), (ON, 5), (Y, 1, 4, 5), (OVER, 3), (SCATTER, 3), (ON, 6), (OVER, 4),
    (RELAY, 1, 0, 1), (CROSS, 0), (ON, 7), (RELAY, 1, 1, 2), (Y, 2, 1, 2), (OVER, 5), (FAR, 11),
    (Y, 2, 2, 3), (ON, 8), (OVER, 6), (Y, 2, 3, 4), (FAR, 12), (ON, 9), (Y, 2, 4, 5), (SETTLE, 0),
    (SPLIT, 0), (MUL, 0, 0, 2), (FAR, 13), (BACK, 0, 0, 2), (ON, 10), (OVER, 7), (RELAY, 1, 2, 4),
    (OVER, 8), (FAR, 14), (OVER, 9), (FAR, 15), (CROSS, 1), (MUL, 0, 2, 3), (PLANES, 3), (BACK, 0, 2, 3),
    (ON, 11), (OVER, 10), (Y, 3, 0, 1), (ON, 12), (ADD, 0, 0, 2), (RELAY, 2, 0, 2), (ON, 13), (OVER, 11),
    (ON, 14), (RELAY, 2, 2, 3), (OVER, 12), (Y, 3, 1, 2), (RELAY, 2, 3, 4), (CROSS, 2), (ON, 15),
    (Y, 3, 2, 3), (OVER, 13), (SETTLE, 1), (SPLIT, 1), (MUL, 1, 0, 2), (BACK, 1, 0, 2), (OVER, 14),
    (Y, 3, 3, 5), (MUL, 1, 2, 3), (BACK, 1, 2, 3), (OVER, 15), (ADD, 0, 2, 3), (SETTLE, 2), (SPLIT, 2),
    (MUL, 2, 0, 2), (BACK, 2, 0, 2), (CROSS, 3), (RELAY, 3, 0, 2), (MUL, 0, 3, 4), (BACK, 0, 3, 4),
    (MUL, 1, 3, 4), (BACK, 1, 3, 4), (RELAY, 3, 2, 4), (MUL, 2, 2, 4), (BACK, 2, 2, 4), (ADD, 1, 0, 2),
    (ADD, 1, 2, 3), (ADD, 2, 0, 2), (SETTLE, 3), (SPLIT, 3), (MUL, 3, 0, 2), (BACK, 3, 0, 2),
    (MUL, 3, 2, 4), (BACK, 3, 2, 4), (ADD, 0, 3, 4), (ADD, 1, 3, 4), (ADD, 2, 2, 4), (ADD, 3, 0, 2),
    (ADD, 3, 2, 4), (FINISH, 0), (FINISH, 1), (FINISH, 2), (FINISH, 3), (DRAIN,),
)


def bulk_wait(ref, sem):
    pltpu.make_async_copy(ref, ref, sem).wait()


def kernel(
    left_ref, right_ref, out_ref,
    lbuf, s1, ag, braw, bs, asp, cp, cr, fin, outs,
    l_own, a1_send, a1_recv, a2_send, z_recv, relay_recv, plain_recv, far_recv, a3_send,
    b_send, b_own, b_par, b_oth, b_oc,
    c_send, c_recv, x_send, x_recv,
):
    G = GROUPS
    l = lax.axis_index("layer")
    z = lax.axis_index("row")
    q = lax.axis_index("col")
    c = q % 2
    h = (q // 2) % 2
    y = q // 4
    a = 2 * h + l
    rg = s1.shape[3]
    width = s1.shape[4]
    sub_rows = rg * G
    mine = a * 2 + c
    slot = h * 2 + c

    def col_of(yy, hh, cc):
        return yy * 4 + hh * 2 + cc

    def dev(dl=0, dz=0, dy=0, dh=0, dc=0):
        return ((l + dl) % 2, (z + dz) % 8, col_of((y + dy) % 4, (h + dh) % 2, (c + dc) % 2))

    def send(src, dst, send_sem, recv_sem, device):
        pltpu.make_async_remote_copy(
            src_ref=src, dst_ref=dst, send_sem=send_sem, recv_sem=recv_sem,
            device_id=device, device_id_type=MESH,
        ).start()

    partners = set()
    for dx in (0, 1):
        for dy in range(4):
            for dc in range(2):
                partners.add((dx, 0, dy, dx, dc))
    for dz in range(1, 8):
        partners.add((0, dz, 0, 0, 0))
    for dl in range(2):
        for dh in range(2):
            for dc in range(2):
                partners.add((dl, 0, 0, dh, dc))
    partners.discard((0, 0, 0, 0, 0))
    partners = sorted(partners)
    def split(x):
        high = x.astype(jnp.bfloat16)
        return high, (x - high.astype(jnp.float32)).astype(jnp.bfloat16)

    def split_right(which, rows, block):
        cols = pl.ds(pl.multiple_of(block * 128, 128), 128)
        real = braw[which, 0, rows, :]
        imag = braw[which, 1, rows, :]
        for m, x in enumerate((real, imag, real + imag)):
            high, low = split(x)
            bs[m, 0, rows, cols] = high
            bs[m, 1, rows, cols] = low

    depth = braw.shape[2]

    def split_whole(which, block):
        @pl.loop(0, depth // 128)
        def _(i):
            split_right(which, pl.ds(pl.multiple_of(i * 128, 128), 128), block)

    with jax.named_scope("entry"):
        pltpu.make_async_copy(left_ref, lbuf, l_own).start()
        pltpu.make_async_copy(right_ref, braw.at[slot], b_own).start()
        barrier = pltpu.get_barrier_semaphore()
        for partner in partners:
            pl.semaphore_signal(barrier, inc=1, device_id=dev(*partner), device_id_type=MESH)
        bulk_wait(lbuf, l_own)
        bulk_wait(braw.at[slot], b_own)
        split_whole(slot, c)
        pl.semaphore_wait(barrier, len(partners))

    def scatter(g):
        for dx in (1, 0):
            near_set = ((q // 2 - z + 6) % 8) // 4
            at = (2 * h + l) if dx == 0 else (2 * (1 - h) + (1 - l))
            for dy in (2, 1, 3, 0):
                for dc in (1, 0):
                    rows = (at * 2 + (c + dc) % 2) * sub_rows + g * rg
                    src_index = (
                        slice(None),
                        pl.ds(pl.multiple_of(rows, rg), rg),
                        pl.ds(pl.multiple_of(((y + dy) % 4) * width, width), width),
                    )
                    src = lbuf.at[src_index]
                    dst = s1.at[g, q]
                    if (dx, dy, dc) == (0, 0, 0):
                        pltpu.make_async_copy(
                            left_ref.at[src_index], dst, a1_recv.at[g, near_set]
                        ).start()
                    else:
                        send(src, dst, a1_send, a1_recv.at[g, near_set], dev(dx, 0, dy, dx, dc))

    def to_planes(g):
        for i, dz in enumerate(FAR_FIRST):
            if i % 4 == 0:
                bulk_wait(s1.at[g, pl.ds(0, 8)], a1_recv.at[g, i // 4])
            k = (z + dz) % 8
            send(
                s1.at[g, pl.ds(2 * k, 2)], ag.at[g, y, :, :, z], a2_send, z_recv.at[g, min(dz, 8 - dz) - 1], dev(0, dz)
            )
        ag[g, y, :, :, z] = s1[g, pl.ds(2 * z, 2)]

    def along_y(g, first, last):
        for j in range(first, last):
            if j:
                dz = ARRIVAL[ARRIVED[j][0]]
                bulk_wait(ag.at[g, y, :, :, pl.ds(0, len(ARRIVED[j]))], z_recv.at[g, min(dz, 8 - dz) - 1])
            for i in ARRIVED[j]:
                r = (z + ARRIVAL[i]) % 8
                piece = ag.at[g, y, :, :, r]
                src = piece if i else s1.at[g, pl.ds(2 * z, 2)]
                for side, dy in enumerate((1, 3)):
                    sem = relay_recv.at[g, RELAY_OF[i]] if i % 2 == side else plain_recv.at[g, side]
                    send(src, piece, a3_send, sem, dev(0, 0, dy))

    def relay(g, first, last):
        for j in range(first, last):
            back, onward = (3, 1) if j % 2 == 0 else (1, 3)
            origin = (y + back) % 4
            bulk_wait(ag.at[g, origin, :, :, pl.ds(0, 2)], relay_recv.at[g, j])
            for i in RELAYED[j]:
                piece = ag.at[g, origin, :, :, (z + ARRIVAL[i]) % 8]
                send(piece, piece, a3_send, far_recv.at[g], dev(0, 0, onward))

    def settle(g):
        for side in range(2):
            bulk_wait(ag.at[g, y, :, :, pl.ds(0, 4)], plain_recv.at[g, side])
        bulk_wait(ag.at[g, y], far_recv.at[g])

    half = depth // 2
    quarter = half // 2
    each = CHUNKS // 2
    chunk = quarter // each

    def rows_of(which, core, i):
        return pl.ds(pl.multiple_of(which * half + core * quarter + (i % each) * chunk, chunk), chunk)

    def quarter_of(which, core):
        return pl.ds(pl.multiple_of(which * half + core * quarter, quarter), quarter)

    def near():
        for which, core in ((1 - l, 1 - c), (1 - l, c), (l, 1 - c), (l, c)):
            piece = braw.at[slot, :, quarter_of(which, core)]
            send(piece, piece, b_send, b_par.at[which, core], dev(dc=1))

    near_other = h * 2 + 1 - c

    seen = []

    def first_quarter():
        if not seen:
            bulk_wait(braw.at[near_other, :, quarter_of(1 - l, c)], b_par.at[1 - l, c])
            seen.append(True)

    def far(i):
        first_quarter()
        piece = braw.at[h * 2 + i // each, :, rows_of(1 - l, c, i)]
        send(piece, piece, b_send, b_oth.at[0, i], dev(1, 0, 0, 1, 0))

    def partner():
        first_quarter()
        for which, core in ((1 - l, 1 - c), (l, c), (l, 1 - c)):
            bulk_wait(braw.at[near_other, :, quarter_of(which, core)], b_par.at[which, core])
        split_whole(near_other, 1 - c)

    def on(i):
        which = (1 - h) * 2 + i // each
        rows = rows_of(l, c, i)
        piece = braw.at[which, :, rows]
        bulk_wait(piece, b_oth.at[0, i])
        send(piece, piece, b_send, b_oth.at[1, i], dev(dl=1))
        send(piece, piece, b_send, b_oc.at[0, i // 4], dev(dc=1))
        split_right(which, rows, 2 + i // each)

    def over(i):
        which = (1 - h) * 2 + i // each
        rows = rows_of(1 - l, c, i)
        piece = braw.at[which, :, rows]
        bulk_wait(piece, b_oth.at[1, i])
        send(piece, piece, b_send, b_oc.at[1, i // 4], dev(dc=1))
        split_right(which, rows, 2 + i // each)

    def cross(i):
        which = (1 - h) * 2 + 4 * i // each
        for k in range(2):
            start = (l if k == 0 else 1 - l) * half + (1 - c) * quarter + (4 * i % each) * chunk
            rows = pl.ds(pl.multiple_of(start, chunk), 4 * chunk)
            bulk_wait(braw.at[which, :, rows], b_oc.at[k, i])
            split_right(which, rows, 2 + 4 * i // each)

    lines = 8 * rg

    def split_left(g):
        for t in range(8):
            for_k, from_y = t // 4, t % 4
            real = ag[g, from_y, for_k, 0].reshape(lines, width)
            imag = ag[g, from_y, for_k, 1].reshape(lines, width)
            for m, x in enumerate((real, imag, real + imag)):
                high, low = split(x)
                asp[g, m, :lines, t * width:(t + 1) * width] = high
                asp[g, m, lines:, t * width:(t + 1) * width] = low

    def multiply(g, lo, hi):
        cols = slice(lo * 128, hi * 128)
        terms = []
        for m in range(3):
            both = jnp.dot(asp[g, m], bs[m, 0, :, cols], preferred_element_type=jnp.float32)
            rest = jnp.dot(asp[g, m, :lines], bs[m, 1, :, cols], preferred_element_type=jnp.float32)
            terms.append(both[:lines] + both[lines:] + rest)
        first, second, third = terms
        for part, x in enumerate((first - second, third - first - second)):
            for b in range(lo, hi):
                cp[g, b, :, part] = x[:, (b - lo) * 128:(b - lo + 1) * 128].reshape(8, rg, 128)

    def hand_back(g, lo, hi):
        blocks = pl.ds(lo, hi - lo)
        for dz in FAR_FIRST:
            r = (z + dz) % 8
            send(cp.at[g, blocks, r], cr.at[g, blocks, z], c_send, c_recv.at[g, lo], dev(0, dz))

    def add_up(g, lo, hi):
        blocks = pl.ds(lo, hi - lo)
        bulk_wait(cr.at[g, blocks, pl.ds(0, 7)], c_recv.at[g, lo])
        total = cp[g, blocks, z]
        for dz in FAR_FIRST:
            total = total + cr[g, blocks, (z + dz) % 8]
        fin[g, lo:hi] = total
        for b in range(lo, hi):
            for dl in (1, 0):
                if b >= 2:
                    target = (l + dl) % 2, z, col_of(y, 1 - h, b - 2)
                    send(fin.at[g, b], outs.at[g, mine], x_send, x_recv.at[g], target)
                else:
                    dc = b
                    if dl or dc:
                        send(
                            fin.at[g, (c + dc) % 2], outs.at[g, mine], x_send, x_recv.at[g],
                            dev(dl, 0, 0, 0, dc),
                        )
        if lo == 0:
            outs[g, mine] = fin[g, c]

    def finish(g):
        bulk_wait(outs.at[g, pl.ds(0, 7)], x_recv.at[g])
        for i in range(8):
            out_ref[:, i * sub_rows + g * rg:i * sub_rows + (g + 1) * rg, :] = outs[g, i]

    def drain():
        bulk_wait(s1.at[:, pl.ds(0, 15)], a1_send)
        bulk_wait(s1.at[:, pl.ds(0, 14)], a2_send)
        bulk_wait(ag.at[:, pl.ds(0, 3)], a3_send)
        bulk_wait(cr.at[:, :, pl.ds(0, 7)], c_send)
        bulk_wait(outs.at[:, pl.ds(0, 7)], x_send)
        bulk_wait(braw.at[pl.ds(0, 3)], b_send)

    calls = (
        scatter, near, far, partner, to_planes, along_y, relay, on, over, cross,
        settle, split_left, multiply, hand_back, add_up, finish, drain,
    )
    for code, *numbers in ORDER:
        with jax.named_scope("_".join([calls[code].__name__, *map(str, numbers)])):
            calls[code](*numbers)


def local(left_matrix, right_matrix):
    _, rows, left_width = left_matrix.shape
    _, depth, cols = right_matrix.shape
    G = GROUPS
    rg = rows // 8 // G
    width = left_width // 4
    f32, bf16 = jnp.float32, jnp.bfloat16
    dma = pltpu.SemaphoreType.DMA
    return pl.pallas_call(
        kernel,
        out_shape=jax.ShapeDtypeStruct((2, rows, cols), f32),
        in_specs=[pl.BlockSpec(memory_space=pl.ANY)] * 2,
        out_specs=pl.BlockSpec(memory_space=pltpu.VMEM),
        scratch_shapes=[
            pltpu.VMEM((2, rows, left_width), f32),
            pltpu.VMEM((G, 16, 2, rg, width), f32),
            pltpu.VMEM((G, 4, 2, 2, 8, rg, width), f32),
            pltpu.VMEM((4, 2, depth, cols), f32),
            pltpu.VMEM((3, 2, depth, 4 * cols), bf16),
            pltpu.VMEM((G, 3, 16 * rg, depth), bf16),
            pltpu.VMEM((G, 4, 8, 2, rg, cols), f32),
            pltpu.VMEM((G, 4, 8, 2, rg, cols), f32),
            pltpu.VMEM((G, 4, 2, rg, cols), f32),
            pltpu.VMEM((G, 8, 2, rg, cols), f32),
            dma, dma, dma((G, 2)), dma, dma((G, 4)), dma((G, 4)), dma((G, 2)), dma((G,)), dma,
            dma, dma, dma((2, 2)), dma((2, CHUNKS)), dma((2, CHUNKS // 4)),
            dma, dma((G, 4)), dma, dma((G,)),
        ],
        compiler_params=pltpu.CompilerParams(
            collective_id=0, has_side_effects=True, vmem_limit_bytes=60 * 1024 * 1024
        ),
    )(left_matrix, right_matrix)


def solution(mesh):
    spec = P(None, "row", "col")
    return jax.shard_map(local, mesh=mesh, in_specs=(spec, spec), out_specs=spec, check_vma=False)
```

```python
import functools

import jax
import jax.numpy as jnp
from jax import lax
from jax.experimental import pallas as pl
from jax.experimental.pallas import tpu as pltpu
from jax.sharding import PartitionSpec as P

MESH = pl.DeviceIdType.MESH
GROUPS = 4
FAR_FIRST = (4, 3, 5, 2, 6, 1, 7)
ARRIVAL = (0, *FAR_FIRST)
ARRIVED = ((0,), (1,), (2, 3), (4, 5), (6, 7))
RELAYED = ((0, 2), (1, 3), (4, 6), (5, 7))
RELAY_OF = {i: j for j, pair in enumerate(RELAYED) for i in pair}
CHUNKS = 16


SCATTER, NEAR, FAR, PARTNER, PLANES, Y, RELAY, ON, OVER, CROSS, SETTLE, SPLIT, MUL, BACK, ADD, FINISH, DRAIN = range(17)
PARTS = (((0, 2), (2, 3), (3, 4)), ((0, 2), (2, 3), (3, 4)), ((0, 2), (2, 3), (3, 4)), ((0, 2), (2, 4)))
ORDER = (
    (SCATTER, 0), (NEAR,), (SCATTER, 1), (FAR, 0), (FAR, 1), (FAR, 2), (SCATTER, 2), (PARTNER,),
    (PLANES, 0), (Y, 0, 0, 1), (FAR, 3), (FAR, 4), (PLANES, 1), (Y, 1, 0, 1), (ON, 0), (FAR, 5),
    (SCATTER, 3), (ON, 1), (Y, 0, 1, 3), (ON, 2), (Y, 0, 3, 4), (OVER, 0), (Y, 0, 4, 5), (FAR, 6),
    (OVER, 1), (FAR, 7), (PLANES, 2), (OVER, 2), (Y, 2, 0, 1), (ON, 3), (RELAY, 0, 0, 1), (FAR, 8),
    (RELAY, 0, 1, 2), (ON, 4), (FAR, 9), (Y, 1, 1, 3), (ON, 5), (RELAY, 0, 2, 3), (FAR, 10),
    (RELAY, 0, 3, 4), (OVER, 3), (FAR, 11), (OVER, 4), (Y, 1, 3, 4), (CROSS, 0), (FAR, 12), (PLANES, 3),
    (OVER, 5), (Y, 1, 4, 5), (ON, 6), (RELAY, 1, 0, 1), (FAR, 13), (RELAY, 1, 1, 2), (ON, 7), (FAR, 14),
    (SETTLE, 0), (SPLIT, 0), (MUL, 0, 0, 2), (FAR, 15), (BACK, 0, 0, 2), (ON, 8), (OVER, 6),
    (Y, 2, 1, 3), (RELAY, 1, 2, 3), (ON, 9), (RELAY, 1, 3, 4), (OVER, 7), (ON, 10), (Y, 2, 3, 4),
    (ON, 11), (CROSS, 1), (MUL, 0, 2, 3), (BACK, 0, 2, 3), (OVER, 8), (Y, 2, 4, 5), (ON, 12),
    (RELAY, 2, 0, 2), (OVER, 9), (ON, 13), (SETTLE, 1), (SPLIT, 1), (MUL, 1, 0, 2), (BACK, 1, 0, 2),
    (ON, 14), (OVER, 10), (Y, 3, 0, 2), (MUL, 1, 2, 3), (BACK, 1, 2, 3), (ON, 15), (OVER, 11),
    (RELAY, 2, 2, 4), (OVER, 12), (Y, 3, 2, 3), (OVER, 13), (CROSS, 2), (Y, 3, 3, 4), (OVER, 14),
    (Y, 3, 4, 5), (SETTLE, 2), (SPLIT, 2), (MUL, 2, 0, 2), (BACK, 2, 0, 2), (OVER, 15), (RELAY, 3, 0, 2),
    (MUL, 2, 2, 3), (BACK, 2, 2, 3), (CROSS, 3), (RELAY, 3, 2, 3), (MUL, 0, 3, 4), (BACK, 0, 3, 4),
    (RELAY, 3, 3, 4), (MUL, 1, 3, 4), (BACK, 1, 3, 4), (MUL, 2, 3, 4), (BACK, 2, 3, 4), (SETTLE, 3),
    (SPLIT, 3), (MUL, 3, 0, 2), (BACK, 3, 0, 2), (MUL, 3, 2, 4), (BACK, 3, 2, 4), (ADD, 0, 0, 2),
    (ADD, 0, 2, 3), (ADD, 1, 0, 2), (ADD, 1, 2, 3), (ADD, 2, 0, 2), (ADD, 2, 2, 3), (ADD, 0, 3, 4),
    (ADD, 1, 3, 4), (ADD, 2, 3, 4), (ADD, 3, 0, 2), (ADD, 3, 2, 4), (FINISH, 0), (FINISH, 1),
    (FINISH, 2), (FINISH, 3), (DRAIN,),
)


def bulk_wait(ref, sem):
    pltpu.make_async_copy(ref, ref, sem).wait()


def kernel(
    left_ref, right_ref, out_ref,
    lbuf, s1, ag, braw, bs, asp, cp, cr, fin, outs,
    l_own, a1_send, a1_recv, a2_send, z_recv, relay_recv, plain_recv, far_recv, a3_send,
    b_send, b_own, b_par, b_oth, b_oc,
    c_send, c_recv, x_send, x_recv,
):
    G = GROUPS
    l = lax.axis_index("layer")
    z = lax.axis_index("row")
    q = lax.axis_index("col")
    c = q % 2
    h = (q // 2) % 2
    y = q // 4
    a = 2 * h + l
    rg = s1.shape[3]
    width = s1.shape[4]
    sub_rows = rg * G
    mine = a * 2 + c
    slot = h * 2 + c

    def col_of(yy, hh, cc):
        return yy * 4 + hh * 2 + cc

    def dev(dl=0, dz=0, dy=0, dh=0, dc=0):
        return ((l + dl) % 2, (z + dz) % 8, col_of((y + dy) % 4, (h + dh) % 2, (c + dc) % 2))

    def send(src, dst, send_sem, recv_sem, device):
        pltpu.make_async_remote_copy(
            src_ref=src, dst_ref=dst, send_sem=send_sem, recv_sem=recv_sem,
            device_id=device, device_id_type=MESH,
        ).start()

    partners = set()
    for dx in (0, 1):
        for dy in range(4):
            for dc in range(2):
                partners.add((dx, 0, dy, dx, dc))
    for dz in range(1, 8):
        partners.add((0, dz, 0, 0, 0))
    for dl in range(2):
        for dh in range(2):
            for dc in range(2):
                partners.add((dl, 0, 0, dh, dc))
    partners.discard((0, 0, 0, 0, 0))
    partners = sorted(partners)
    def split(x):
        high = x.astype(jnp.bfloat16)
        return high, (x - high.astype(jnp.float32)).astype(jnp.bfloat16)

    def split_right(which, rows, block):
        cols = pl.ds(pl.multiple_of(block * 128, 128), 128)
        real = braw[which, 0, rows, :]
        imag = braw[which, 1, rows, :]
        for m, x in enumerate((real, imag, real + imag)):
            high, low = split(x)
            bs[m, 0, rows, cols] = high
            bs[m, 1, rows, cols] = low

    depth = braw.shape[2]

    def split_whole(which, block):
        @pl.loop(0, depth // 128)
        def _(i):
            split_right(which, pl.ds(pl.multiple_of(i * 128, 128), 128), block)

    with jax.named_scope("entry"):
        pltpu.make_async_copy(left_ref, lbuf, l_own).start()
        pltpu.make_async_copy(right_ref, braw.at[slot], b_own).start()
        barrier = pltpu.get_barrier_semaphore()
        for partner in partners:
            pl.semaphore_signal(barrier, inc=1, device_id=dev(*partner), device_id_type=MESH)
        bulk_wait(lbuf, l_own)
        bulk_wait(braw.at[slot], b_own)
        split_whole(slot, c)
        pl.semaphore_wait(barrier, len(partners))

    def scatter(g):
        for dx in (1, 0):
            near_set = ((q // 2 - z + 6) % 8) // 4
            at = (2 * h + l) if dx == 0 else (2 * (1 - h) + (1 - l))
            for dy in (2, 1, 3, 0):
                for dc in (1, 0):
                    rows = (at * 2 + (c + dc) % 2) * sub_rows + g * rg
                    src_index = (
                        slice(None),
                        pl.ds(pl.multiple_of(rows, rg), rg),
                        pl.ds(pl.multiple_of(((y + dy) % 4) * width, width), width),
                    )
                    src = lbuf.at[src_index]
                    dst = s1.at[g, q]
                    if (dx, dy, dc) == (0, 0, 0):
                        pltpu.make_async_copy(
                            left_ref.at[src_index], dst, a1_recv.at[g, near_set]
                        ).start()
                    else:
                        send(src, dst, a1_send, a1_recv.at[g, near_set], dev(dx, 0, dy, dx, dc))

    def to_planes(g):
        for i, dz in enumerate(FAR_FIRST):
            if i % 4 == 0:
                bulk_wait(s1.at[g, pl.ds(0, 8)], a1_recv.at[g, i // 4])
            k = (z + dz) % 8
            send(
                s1.at[g, pl.ds(2 * k, 2)], ag.at[g, y, :, :, z], a2_send, z_recv.at[g, min(dz, 8 - dz) - 1], dev(0, dz)
            )
        ag[g, y, :, :, z] = s1[g, pl.ds(2 * z, 2)]

    def along_y(g, first, last):
        for j in range(first, last):
            if j:
                dz = ARRIVAL[ARRIVED[j][0]]
                bulk_wait(ag.at[g, y, :, :, pl.ds(0, len(ARRIVED[j]))], z_recv.at[g, min(dz, 8 - dz) - 1])
            for i in ARRIVED[j]:
                r = (z + ARRIVAL[i]) % 8
                piece = ag.at[g, y, :, :, r]
                src = piece if i else s1.at[g, pl.ds(2 * z, 2)]
                for side, dy in enumerate((1, 3)):
                    sem = relay_recv.at[g, RELAY_OF[i]] if i % 2 == side else plain_recv.at[g, side]
                    send(src, piece, a3_send, sem, dev(0, 0, dy))

    def relay(g, first, last):
        for j in range(first, last):
            back, onward = (3, 1) if j % 2 == 0 else (1, 3)
            origin = (y + back) % 4
            bulk_wait(ag.at[g, origin, :, :, pl.ds(0, 2)], relay_recv.at[g, j])
            for i in RELAYED[j]:
                piece = ag.at[g, origin, :, :, (z + ARRIVAL[i]) % 8]
                send(piece, piece, a3_send, far_recv.at[g], dev(0, 0, onward))

    def settle(g):
        for side in range(2):
            bulk_wait(ag.at[g, y, :, :, pl.ds(0, 4)], plain_recv.at[g, side])
        bulk_wait(ag.at[g, y], far_recv.at[g])

    half = depth // 2
    quarter = half // 2
    each = CHUNKS // 2
    chunk = quarter // each

    def rows_of(which, core, i):
        return pl.ds(pl.multiple_of(which * half + core * quarter + (i % each) * chunk, chunk), chunk)

    def quarter_of(which, core):
        return pl.ds(pl.multiple_of(which * half + core * quarter, quarter), quarter)

    def near():
        for which, core in ((1 - l, 1 - c), (1 - l, c), (l, 1 - c), (l, c)):
            piece = braw.at[slot, :, quarter_of(which, core)]
            send(piece, piece, b_send, b_par.at[which, core], dev(dc=1))

    near_other = h * 2 + 1 - c

    seen = []

    def first_quarter():
        if not seen:
            bulk_wait(braw.at[near_other, :, quarter_of(1 - l, c)], b_par.at[1 - l, c])
            seen.append(True)

    def far(i):
        first_quarter()
        piece = braw.at[h * 2 + i // each, :, rows_of(1 - l, c, i)]
        send(piece, piece, b_send, b_oth.at[0, i], dev(1, 0, 0, 1, 0))

    def partner():
        first_quarter()
        for which, core in ((1 - l, 1 - c), (l, c), (l, 1 - c)):
            bulk_wait(braw.at[near_other, :, quarter_of(which, core)], b_par.at[which, core])
        split_whole(near_other, 1 - c)

    def on(i):
        which = (1 - h) * 2 + i // each
        rows = rows_of(l, c, i)
        piece = braw.at[which, :, rows]
        bulk_wait(piece, b_oth.at[0, i])
        send(piece, piece, b_send, b_oth.at[1, i], dev(dl=1))
        send(piece, piece, b_send, b_oc.at[0, i // 4], dev(dc=1))
        split_right(which, rows, 2 + i // each)

    def over(i):
        which = (1 - h) * 2 + i // each
        rows = rows_of(1 - l, c, i)
        piece = braw.at[which, :, rows]
        bulk_wait(piece, b_oth.at[1, i])
        send(piece, piece, b_send, b_oc.at[1, i // 4], dev(dc=1))
        split_right(which, rows, 2 + i // each)

    def cross(i):
        which = (1 - h) * 2 + 4 * i // each
        for k in range(2):
            start = (l if k == 0 else 1 - l) * half + (1 - c) * quarter + (4 * i % each) * chunk
            rows = pl.ds(pl.multiple_of(start, chunk), 4 * chunk)
            bulk_wait(braw.at[which, :, rows], b_oc.at[k, i])
            split_right(which, rows, 2 + 4 * i // each)

    lines = 8 * rg

    def split_left(g):
        for t in range(8):
            for_k, from_y = t // 4, t % 4
            real = ag[g, from_y, for_k, 0].reshape(lines, width)
            imag = ag[g, from_y, for_k, 1].reshape(lines, width)
            for m, x in enumerate((real, imag, real + imag)):
                high, low = split(x)
                asp[g, m, :lines, t * width:(t + 1) * width] = high
                asp[g, m, lines:, t * width:(t + 1) * width] = low

    def multiply(g, lo, hi):
        cols = slice(lo * 128, hi * 128)
        terms = []
        for m in range(3):
            both = jnp.dot(asp[g, m], bs[m, 0, :, cols], preferred_element_type=jnp.float32)
            rest = jnp.dot(asp[g, m, :lines], bs[m, 1, :, cols], preferred_element_type=jnp.float32)
            terms.append(both[:lines] + both[lines:] + rest)
        first, second, third = terms
        for part, x in enumerate((first - second, third - first - second)):
            for b in range(lo, hi):
                cp[g, b, :, part] = x[:, (b - lo) * 128:(b - lo + 1) * 128].reshape(8, rg, 128)

    def hand_back(g, lo, hi):
        blocks = pl.ds(lo, hi - lo)
        for dz in FAR_FIRST:
            r = (z + dz) % 8
            send(cp.at[g, blocks, r], cr.at[g, blocks, z], c_send, c_recv.at[g, lo], dev(0, dz))

    def add_up(g, lo, hi):
        blocks = pl.ds(lo, hi - lo)
        bulk_wait(cr.at[g, blocks, pl.ds(0, 7)], c_recv.at[g, lo])
        total = cp[g, blocks, z]
        for dz in FAR_FIRST:
            total = total + cr[g, blocks, (z + dz) % 8]
        fin[g, lo:hi] = total
        for b in range(lo, hi):
            for dl in (1, 0):
                if b >= 2:
                    target = (l + dl) % 2, z, col_of(y, 1 - h, b - 2)
                    send(fin.at[g, b], outs.at[g, mine], x_send, x_recv.at[g], target)
                else:
                    dc = b
                    if dl or dc:
                        send(
                            fin.at[g, (c + dc) % 2], outs.at[g, mine], x_send, x_recv.at[g],
                            dev(dl, 0, 0, 0, dc),
                        )
        if lo == 0:
            outs[g, mine] = fin[g, c]

    def finish(g):
        bulk_wait(outs.at[g, pl.ds(0, 7)], x_recv.at[g])
        for i in range(8):
            out_ref[:, i * sub_rows + g * rg:i * sub_rows + (g + 1) * rg, :] = outs[g, i]

    def drain():
        bulk_wait(s1.at[:, pl.ds(0, 15)], a1_send)
        bulk_wait(s1.at[:, pl.ds(0, 14)], a2_send)
        bulk_wait(ag.at[:, pl.ds(0, 3)], a3_send)
        bulk_wait(cr.at[:, :, pl.ds(0, 7)], c_send)
        bulk_wait(outs.at[:, pl.ds(0, 7)], x_send)
        bulk_wait(braw.at[pl.ds(0, 3)], b_send)

    calls = (
        scatter, near, far, partner, to_planes, along_y, relay, on, over, cross,
        settle, split_left, multiply, hand_back, add_up, finish, drain,
    )
    for code, *numbers in ORDER:
        with jax.named_scope("_".join([calls[code].__name__, *map(str, numbers)])):
            calls[code](*numbers)


def local(left_matrix, right_matrix):
    _, rows, left_width = left_matrix.shape
    _, depth, cols = right_matrix.shape
    G = GROUPS
    rg = rows // 8 // G
    width = left_width // 4
    f32, bf16 = jnp.float32, jnp.bfloat16
    dma = pltpu.SemaphoreType.DMA
    return pl.pallas_call(
        kernel,
        out_shape=pltpu.VMEM((2, rows, cols), f32),
        in_specs=[pl.BlockSpec(memory_space=pl.ANY)] * 2,
        out_specs=pl.BlockSpec(memory_space=pltpu.VMEM),
        scratch_shapes=[
            pltpu.VMEM((2, rows, left_width), f32),
            pltpu.VMEM((G, 16, 2, rg, width), f32),
            pltpu.VMEM((G, 4, 2, 2, 8, rg, width), f32),
            pltpu.VMEM((4, 2, depth, cols), f32),
            pltpu.VMEM((3, 2, depth, 4 * cols), bf16),
            pltpu.VMEM((G, 3, 16 * rg, depth), bf16),
            pltpu.VMEM((G, 4, 8, 2, rg, cols), f32),
            pltpu.VMEM((G, 4, 8, 2, rg, cols), f32),
            pltpu.VMEM((G, 4, 2, rg, cols), f32),
            pltpu.VMEM((G, 8, 2, rg, cols), f32),
            dma, dma, dma((G, 2)), dma, dma((G, 4)), dma((G, 4)), dma((G, 2)), dma((G,)), dma,
            dma, dma, dma((2, 2)), dma((2, CHUNKS)), dma((2, CHUNKS // 4)),
            dma, dma((G, 4)), dma, dma((G,)),
        ],
        compiler_params=pltpu.CompilerParams(
            collective_id=0, has_side_effects=True, vmem_limit_bytes=60 * 1024 * 1024
        ),
    )(left_matrix, right_matrix)


def solution(mesh):
    spec = P(None, "row", "col")
    return jax.shard_map(local, mesh=mesh, in_specs=(spec, spec), out_specs=spec, check_vma=False)
```

```python
import functools

import jax
import jax.numpy as jnp
from jax import lax
from jax.experimental import pallas as pl
from jax.experimental.pallas import tpu as pltpu
from jax.sharding import PartitionSpec as P

MESH = pl.DeviceIdType.MESH
GROUPS = 4
FAR_FIRST = (4, 3, 5, 2, 6, 1, 7)
ARRIVAL = (0, *FAR_FIRST)
ARRIVED = ((0,), (1,), (2, 3), (4, 5), (6, 7))
RELAYED = ((0, 2), (1, 3), (4, 6), (5, 7))
SPREAD = (0, 1, 3, 2)
RELAY_OF = {i: j for j, pair in enumerate(RELAYED) for i in pair}
CHUNKS = 16


SCATTER, NEAR, FAR, PARTNER, PLANES, Y, RELAY, ON, OVER, CROSS, SETTLE, SPLIT, MUL, BACK, ADD, FINISH, DRAIN, PLAIN, EARLY, HEAD = range(20)
PARTS = (((0, 2), (2, 3), (3, 4)), ((0, 2), (2, 3), (3, 4)), ((0, 2), (2, 3), (3, 4)), ((0, 2), (2, 4)))
ORDER = (
    (SCATTER, 0), (NEAR,), (SCATTER, 1), (SCATTER, 2), (PARTNER,), (PLANES, 0), (Y, 0, 0, 1), (FAR, 0),
    (SCATTER, 3), (PLANES, 1), (Y, 1, 0, 1), (FAR, 1), (Y, 0, 1, 2), (PLANES, 2), (Y, 2, 0, 1), (FAR, 2),
    (Y, 0, 2, 3), (ON, 0), (Y, 0, 3, 4), (FAR, 3), (Y, 0, 4, 5), (PLAIN, 0), (FAR, 4), (PLANES, 3),
    (OVER, 0), (FAR, 5), (ON, 1), (RELAY, 0, 0, 2), (Y, 1, 1, 2), (FAR, 6), (Y, 1, 2, 3), (ON, 2),
    (RELAY, 0, 2, 4), (Y, 1, 3, 4), (FAR, 7), (ON, 3), (Y, 1, 4, 5), (OVER, 1), (FAR, 8), (ON, 4),
    (OVER, 2), (FAR, 9), (PLAIN, 1), (ON, 5), (RELAY, 1, 0, 2), (OVER, 3), (FAR, 10), (ON, 6),
    (SETTLE, 0), (SPLIT, 0), (OVER, 4), (FAR, 11), (ON, 7), (CROSS, 0), (RELAY, 1, 2, 4), (OVER, 5),
    (FAR, 12), (ON, 8), (MUL, 0, 0, 2), (FAR, 13), (BACK, 0, 0, 2), (ON, 9), (OVER, 6), (Y, 2, 1, 5),
    (OVER, 7), (FAR, 14), (ON, 10), (PLAIN, 2), (OVER, 8), (FAR, 15), (ON, 11), (CROSS, 1),
    (MUL, 0, 2, 3), (BACK, 0, 2, 3), (ON, 12), (OVER, 9), (RELAY, 2, 0, 2), (SETTLE, 1), (SPLIT, 1),
    (MUL, 1, 0, 2), (BACK, 1, 0, 2), (ON, 13), (OVER, 10), (RELAY, 2, 2, 4), (OVER, 11), (ON, 14),
    (MUL, 1, 2, 3), (BACK, 1, 2, 3), (OVER, 12), (Y, 3, 0, 1), (ON, 15), (CROSS, 2), (Y, 3, 1, 4),
    (OVER, 13), (Y, 3, 4, 5), (PLAIN, 3), (OVER, 14), (SETTLE, 2), (SPLIT, 2), (MUL, 2, 0, 2),
    (BACK, 2, 0, 2), (OVER, 15), (RELAY, 3, 0, 2), (MUL, 2, 2, 3), (BACK, 2, 2, 3), (RELAY, 3, 2, 4),
    (CROSS, 3), (MUL, 0, 3, 4), (BACK, 0, 3, 4), (MUL, 1, 3, 4), (BACK, 1, 3, 4), (EARLY, 3),
    (MUL, 2, 3, 4), (BACK, 2, 3, 4), (HEAD, 3, 2, 4), (HEAD, 3, 0, 2), (SETTLE, 3), (SPLIT, 3),
    (MUL, 3, 2, 4), (BACK, 3, 2, 4), (MUL, 3, 0, 2), (BACK, 3, 0, 2), (ADD, 0, 0, 2), (ADD, 0, 2, 3),
    (ADD, 1, 0, 2), (ADD, 1, 2, 3), (ADD, 2, 0, 2), (ADD, 2, 2, 3), (ADD, 0, 3, 4), (ADD, 1, 3, 4),
    (ADD, 2, 3, 4), (ADD, 3, 2, 4), (ADD, 3, 0, 2), (FINISH, 0), (FINISH, 1), (FINISH, 2), (FINISH, 3),
    (DRAIN,),
)


def bulk_wait(ref, sem):
    pltpu.make_async_copy(ref, ref, sem).wait()


def kernel(
    left_ref, right_ref, out_ref,
    lbuf, s1, ag, braw, bs, asp, cp, cr, fin, outs, head,
    l_own, a1_send, a1_recv, a2_send, z_recv, relay_recv, plain_recv, far_recv, a3_send,
    b_send, b_own, b_par, b_oth, b_oc,
    c_send, c_recv, x_send, x_recv,
):
    G = GROUPS
    l = lax.axis_index("layer")
    z = lax.axis_index("row")
    q = lax.axis_index("col")
    c = q % 2
    h = (q // 2) % 2
    y = q // 4
    a = 2 * h + l
    rg = s1.shape[3]
    width = s1.shape[4]
    sub_rows = rg * G
    mine = a * 2 + c
    slot = h * 2 + c

    def col_of(yy, hh, cc):
        return yy * 4 + hh * 2 + cc

    def dev(dl=0, dz=0, dy=0, dh=0, dc=0):
        return ((l + dl) % 2, (z + dz) % 8, col_of((y + dy) % 4, (h + dh) % 2, (c + dc) % 2))

    def send(src, dst, send_sem, recv_sem, device):
        pltpu.make_async_remote_copy(
            src_ref=src, dst_ref=dst, send_sem=send_sem, recv_sem=recv_sem,
            device_id=device, device_id_type=MESH,
        ).start()

    partners = set()
    for dx in (0, 1):
        for dy in range(4):
            for dc in range(2):
                partners.add((dx, 0, dy, dx, dc))
    for dz in range(1, 8):
        partners.add((0, dz, 0, 0, 0))
    for dl in range(2):
        for dh in range(2):
            for dc in range(2):
                partners.add((dl, 0, 0, dh, dc))
    partners.discard((0, 0, 0, 0, 0))
    partners = sorted(partners)
    def split(x):
        high = x.astype(jnp.bfloat16)
        return high, (x - high.astype(jnp.float32)).astype(jnp.bfloat16)

    def split_right(which, start, size, block):
        rows = pl.ds(pl.multiple_of(start, size), size)
        tile = start // 256
        away = (tile % 4 - y + 4) % 4
        place = away + away // 2 - 2 * (away // 3)
        into = pl.ds(pl.multiple_of((place * 2 + tile // 4) * 256 + start % 256, size), size)
        cols = pl.ds(pl.multiple_of(block * 128, 128), 128)
        real = braw[which, 0, rows, :]
        imag = braw[which, 1, rows, :]
        for m, x in enumerate((real, imag, real + imag)):
            high, low = split(x)
            bs[m, 0, into, cols] = high
            bs[m, 1, into, cols] = low

    depth = braw.shape[2]

    def split_whole(which, block):
        @pl.loop(0, depth // 128)
        def _(i):
            split_right(which, i * 128, 128, block)

    with jax.named_scope("entry"):
        pltpu.make_async_copy(left_ref, lbuf, l_own).start()
        pltpu.make_async_copy(right_ref, braw.at[slot], b_own).start()
        barrier = pltpu.get_barrier_semaphore()
        for partner in partners:
            pl.semaphore_signal(barrier, inc=1, device_id=dev(*partner), device_id_type=MESH)
        bulk_wait(lbuf, l_own)
        bulk_wait(braw.at[slot], b_own)
        split_whole(slot, c)
        pl.semaphore_wait(barrier, len(partners))

    def scatter(g):
        for dx in (1, 0):
            near_set = ((q // 2 - z + 6) % 8) // 4
            at = (2 * h + l) if dx == 0 else (2 * (1 - h) + (1 - l))
            for dy in (2, 1, 3, 0):
                for dc in (1, 0):
                    rows = (at * 2 + (c + dc) % 2) * sub_rows + g * rg
                    src_index = (
                        slice(None),
                        pl.ds(pl.multiple_of(rows, rg), rg),
                        pl.ds(pl.multiple_of(((y + dy) % 4) * width, width), width),
                    )
                    src = lbuf.at[src_index]
                    dst = s1.at[g, q]
                    if (dx, dy, dc) == (0, 0, 0):
                        pltpu.make_async_copy(
                            left_ref.at[src_index], dst, a1_recv.at[g, near_set]
                        ).start()
                    else:
                        send(src, dst, a1_send, a1_recv.at[g, near_set], dev(dx, 0, dy, dx, dc))

    def to_planes(g):
        for i, dz in enumerate(FAR_FIRST):
            if i % 4 == 0:
                bulk_wait(s1.at[g, pl.ds(0, 8)], a1_recv.at[g, i // 4])
            k = (z + dz) % 8
            send(
                s1.at[g, pl.ds(2 * k, 2)], ag.at[g, y, :, :, z], a2_send, z_recv.at[g, min(dz, 8 - dz) - 1], dev(0, dz)
            )
        ag[g, y, :, :, z] = s1[g, pl.ds(2 * z, 2)]

    def along_y(g, first, last):
        for j in range(first, last):
            if j:
                dz = ARRIVAL[ARRIVED[j][0]]
                bulk_wait(ag.at[g, y, :, :, pl.ds(0, len(ARRIVED[j]))], z_recv.at[g, min(dz, 8 - dz) - 1])
            for i in ARRIVED[j]:
                r = (z + ARRIVAL[i]) % 8
                piece = ag.at[g, y, :, :, r]
                src = piece if i else s1.at[g, pl.ds(2 * z, 2)]
                send(src, piece, a3_send, relay_recv.at[g, RELAY_OF[i]], dev(0, 0, 1 if i % 2 == 0 else 3))

    def plain(g):
        for i in range(8):
            piece = ag.at[g, y, :, :, (z + ARRIVAL[i]) % 8]
            src = piece if i else s1.at[g, pl.ds(2 * z, 2)]
            side = (i + 1) % 2
            send(src, piece, a3_send, plain_recv.at[g, side], dev(0, 0, (1, 3)[side]))

    def relay(g, first, last):
        for j in range(first, last):
            back, onward = (3, 1) if j % 2 == 0 else (1, 3)
            origin = (y + back) % 4
            bulk_wait(ag.at[g, origin, :, :, pl.ds(0, 2)], relay_recv.at[g, j])
            for i in RELAYED[j]:
                piece = ag.at[g, origin, :, :, (z + ARRIVAL[i]) % 8]
                send(piece, piece, a3_send, far_recv.at[g], dev(0, 0, onward))

    def near_in(g):
        for side in range(2):
            bulk_wait(ag.at[g, y, :, :, pl.ds(0, 4)], plain_recv.at[g, side])

    def settle(g):
        if g < G - 1:
            near_in(g)
        bulk_wait(ag.at[g, y], far_recv.at[g])

    half = depth // 2
    quarter = half // 2
    each = CHUNKS // 2
    chunk = quarter // each

    def start_of(which, core, i):
        return which * half + core * quarter + (i % each) * chunk

    def rows_of(which, core, i):
        return pl.ds(pl.multiple_of(start_of(which, core, i), chunk), chunk)

    def quarter_of(which, core):
        return pl.ds(pl.multiple_of(which * half + core * quarter, quarter), quarter)

    def near():
        for which, core in ((1 - l, 1 - c), (1 - l, c), (l, 1 - c), (l, c)):
            piece = braw.at[slot, :, quarter_of(which, core)]
            send(piece, piece, b_send, b_par.at[which, core], dev(dc=1))

    near_other = h * 2 + 1 - c

    seen = []

    def first_quarter():
        if not seen:
            bulk_wait(braw.at[near_other, :, quarter_of(1 - l, c)], b_par.at[1 - l, c])
            seen.append(True)

    def far(i):
        first_quarter()
        piece = braw.at[h * 2 + i // each, :, rows_of(1 - l, c, i)]
        send(piece, piece, b_send, b_oth.at[0, i], dev(1, 0, 0, 1, 0))

    def partner():
        first_quarter()
        for which, core in ((1 - l, 1 - c), (l, c), (l, 1 - c)):
            bulk_wait(braw.at[near_other, :, quarter_of(which, core)], b_par.at[which, core])
        split_whole(near_other, 1 - c)

    def on(i):
        which = (1 - h) * 2 + i // each
        rows = rows_of(l, c, i)
        piece = braw.at[which, :, rows]
        bulk_wait(piece, b_oth.at[0, i])
        send(piece, piece, b_send, b_oth.at[1, i], dev(dl=1))
        send(piece, piece, b_send, b_oc.at[0, i // 4], dev(dc=1))
        split_right(which, start_of(l, c, i), chunk, 2 + i // each)

    def over(i):
        which = (1 - h) * 2 + i // each
        rows = rows_of(1 - l, c, i)
        piece = braw.at[which, :, rows]
        bulk_wait(piece, b_oth.at[1, i])
        send(piece, piece, b_send, b_oc.at[1, i // 4], dev(dc=1))
        split_right(which, start_of(1 - l, c, i), chunk, 2 + i // each)

    def cross(i):
        which = (1 - h) * 2 + 4 * i // each
        for k in range(2):
            start = (l if k == 0 else 1 - l) * half + (1 - c) * quarter + (4 * i % each) * chunk
            rows = pl.ds(pl.multiple_of(start, chunk), 4 * chunk)
            bulk_wait(braw.at[which, :, rows], b_oc.at[k, i])
            split_right(which, start, 4 * chunk, 2 + 4 * i // each)

    lines = 8 * rg

    def split_tiles(g, first, last):
        for t in range(first, last):
            for_k, from_y = t % 2, (y + SPREAD[t // 2]) % 4
            real = ag[g, from_y, for_k, 0].reshape(lines, width)
            imag = ag[g, from_y, for_k, 1].reshape(lines, width)
            for m, x in enumerate((real, imag, real + imag)):
                high, low = split(x)
                asp[g, m, :lines, t * width:(t + 1) * width] = high
                asp[g, m, lines:, t * width:(t + 1) * width] = low

    def split_left(g):
        split_tiles(g, 0 if g < G - 1 else 6, 8)

    def early(g):
        near_in(g)
        split_tiles(g, 0, 6)

    def dots(g, m, lo, hi, first, last):
        deep, cols = slice(first * width, last * width), slice(lo * 128, hi * 128)
        both = jnp.dot(asp[g, m, :, deep], bs[m, 0, deep, cols], preferred_element_type=jnp.float32)
        rest = jnp.dot(asp[g, m, :lines, deep], bs[m, 1, deep, cols], preferred_element_type=jnp.float32)
        return both[:lines] + both[lines:] + rest

    def begin(g, lo, hi):
        for m in range(3):
            head[m, :, lo * 128:hi * 128] = dots(g, m, lo, hi, 0, 6)

    def multiply(g, lo, hi):
        if g < G - 1:
            first, second, third = (dots(g, m, lo, hi, 0, 8) for m in range(3))
        else:
            first, second, third = (head[m, :, lo * 128:hi * 128] + dots(g, m, lo, hi, 6, 8) for m in range(3))
        for part, x in enumerate((first - second, third - first - second)):
            for b in range(lo, hi):
                cp[g, b, :, part] = x[:, (b - lo) * 128:(b - lo + 1) * 128].reshape(8, rg, 128)

    def hand_back(g, lo, hi):
        blocks = pl.ds(lo, hi - lo)
        for dz in FAR_FIRST:
            r = (z + dz) % 8
            send(cp.at[g, blocks, r], cr.at[g, blocks, z], c_send, c_recv.at[g, lo], dev(0, dz))

    def add_up(g, lo, hi):
        blocks = pl.ds(lo, hi - lo)
        bulk_wait(cr.at[g, blocks, pl.ds(0, 7)], c_recv.at[g, lo])
        total = cp[g, blocks, z]
        for dz in FAR_FIRST:
            total = total + cr[g, blocks, (z + dz) % 8]
        fin[g, lo:hi] = total
        for b in range(lo, hi):
            for dl in (1, 0):
                if b >= 2:
                    target = (l + dl) % 2, z, col_of(y, 1 - h, b - 2)
                    send(fin.at[g, b], outs.at[g, mine], x_send, x_recv.at[g], target)
                else:
                    dc = b
                    if dl or dc:
                        send(
                            fin.at[g, (c + dc) % 2], outs.at[g, mine], x_send, x_recv.at[g],
                            dev(dl, 0, 0, 0, dc),
                        )
        if lo == 0:
            outs[g, mine] = fin[g, c]

    def finish(g):
        bulk_wait(outs.at[g, pl.ds(0, 7)], x_recv.at[g])
        for i in range(8):
            out_ref[:, i * sub_rows + g * rg:i * sub_rows + (g + 1) * rg, :] = outs[g, i]

    def drain():
        bulk_wait(s1.at[:, pl.ds(0, 15)], a1_send)
        bulk_wait(s1.at[:, pl.ds(0, 14)], a2_send)
        bulk_wait(ag.at[:, pl.ds(0, 3)], a3_send)
        bulk_wait(cr.at[:, :, pl.ds(0, 7)], c_send)
        bulk_wait(outs.at[:, pl.ds(0, 7)], x_send)
        bulk_wait(braw.at[pl.ds(0, 3)], b_send)

    calls = (
        scatter, near, far, partner, to_planes, along_y, relay, on, over, cross,
        settle, split_left, multiply, hand_back, add_up, finish, drain, plain, early, begin,
    )
    for code, *numbers in ORDER:
        with jax.named_scope("_".join([calls[code].__name__, *map(str, numbers)])):
            calls[code](*numbers)


def local(left_matrix, right_matrix):
    _, rows, left_width = left_matrix.shape
    _, depth, cols = right_matrix.shape
    G = GROUPS
    rg = rows // 8 // G
    width = left_width // 4
    f32, bf16 = jnp.float32, jnp.bfloat16
    dma = pltpu.SemaphoreType.DMA
    return pl.pallas_call(
        kernel,
        out_shape=pltpu.VMEM((2, rows, cols), f32),
        in_specs=[pl.BlockSpec(memory_space=pl.ANY)] * 2,
        out_specs=pl.BlockSpec(memory_space=pltpu.VMEM),
        scratch_shapes=[
            pltpu.VMEM((2, rows, left_width), f32),
            pltpu.VMEM((G, 16, 2, rg, width), f32),
            pltpu.VMEM((G, 4, 2, 2, 8, rg, width), f32),
            pltpu.VMEM((4, 2, depth, cols), f32),
            pltpu.VMEM((3, 2, depth, 4 * cols), bf16),
            pltpu.VMEM((G, 3, 16 * rg, depth), bf16),
            pltpu.VMEM((G, 4, 8, 2, rg, cols), f32),
            pltpu.VMEM((G, 4, 8, 2, rg, cols), f32),
            pltpu.VMEM((G, 4, 2, rg, cols), f32),
            pltpu.VMEM((G, 8, 2, rg, cols), f32),
            pltpu.VMEM((3, 8 * rg, 4 * cols), f32),
            dma, dma, dma((G, 2)), dma, dma((G, 4)), dma((G, 4)), dma((G, 2)), dma((G,)), dma,
            dma, dma, dma((2, 2)), dma((2, CHUNKS)), dma((2, CHUNKS // 4)),
            dma, dma((G, 4)), dma, dma((G,)),
        ],
        compiler_params=pltpu.CompilerParams(
            collective_id=0, has_side_effects=True, vmem_limit_bytes=60 * 1024 * 1024
        ),
    )(left_matrix, right_matrix)


def solution(mesh):
    spec = P(None, "row", "col")
    return jax.shard_map(local, mesh=mesh, in_specs=(spec, spec), out_specs=spec, check_vma=False)
```

```python
import functools

import jax
import jax.numpy as jnp
from jax import lax
from jax.experimental import pallas as pl
from jax.experimental.pallas import tpu as pltpu
from jax.sharding import PartitionSpec as P

MESH = pl.DeviceIdType.MESH
GROUPS = 4
FAR_FIRST = (4, 3, 5, 2, 6, 1, 7)
ARRIVAL = (0, *FAR_FIRST)
ARRIVED = ((0,), (1,), (2, 3), (4, 5), (6, 7))
RELAYED = ((0, 2), (1, 3), (4, 6), (5, 7))
SPREAD = (0, 1, 3, 2)
RELAY_OF = {i: j for j, pair in enumerate(RELAYED) for i in pair}
CHUNKS = 16


SCATTER, NEAR, FAR, PARTNER, PLANES, Y, RELAY, ON, OVER, CROSS, SETTLE, SPLIT, MUL, BACK, ADD, FINISH, DRAIN, PLAIN, EARLY, HEAD = range(20)
PARTS = (((0, 2), (2, 3), (3, 4)), ((0, 2), (2, 3), (3, 4)), ((0, 2), (2, 3), (3, 4)), ((0, 2), (2, 4)))
ORDER = (
    (SCATTER, 0), (NEAR,), (SCATTER, 1), (SCATTER, 2), (PARTNER,), (PLANES, 0), (Y, 0, 0, 1), (FAR, 0),
    (SCATTER, 3), (PLANES, 1), (Y, 1, 0, 1), (FAR, 1), (Y, 0, 1, 2), (PLANES, 2), (Y, 2, 0, 1), (FAR, 2),
    (Y, 0, 2, 3), (ON, 0), (Y, 0, 3, 4), (FAR, 3), (Y, 0, 4, 5), (PLAIN, 0), (FAR, 4), (PLANES, 3),
    (OVER, 0), (FAR, 5), (ON, 1), (RELAY, 0, 0, 2), (Y, 1, 1, 2), (FAR, 6), (Y, 1, 2, 3), (ON, 2),
    (RELAY, 0, 2, 4), (Y, 1, 3, 4), (FAR, 7), (ON, 3), (Y, 1, 4, 5), (OVER, 1), (FAR, 8), (ON, 4),
    (OVER, 2), (FAR, 9), (PLAIN, 1), (ON, 5), (RELAY, 1, 0, 2), (OVER, 3), (FAR, 10), (ON, 6),
    (SETTLE, 0), (SPLIT, 0), (OVER, 4), (FAR, 11), (ON, 7), (CROSS, 0), (RELAY, 1, 2, 4), (OVER, 5),
    (FAR, 12), (ON, 8), (MUL, 0, 0, 2), (FAR, 13), (BACK, 0, 0, 2), (ON, 9), (OVER, 6), (Y, 2, 1, 5),
    (OVER, 7), (FAR, 14), (ON, 10), (PLAIN, 2), (OVER, 8), (FAR, 15), (ON, 11), (CROSS, 1),
    (MUL, 0, 2, 3), (BACK, 0, 2, 3), (ON, 12), (OVER, 9), (RELAY, 2, 0, 2), (SETTLE, 1), (SPLIT, 1),
    (MUL, 1, 0, 2), (BACK, 1, 0, 2), (ON, 13), (OVER, 10), (RELAY, 2, 2, 4), (OVER, 11), (ON, 14),
    (MUL, 1, 2, 3), (BACK, 1, 2, 3), (OVER, 12), (Y, 3, 0, 1), (ON, 15), (CROSS, 2), (Y, 3, 1, 4),
    (OVER, 13), (Y, 3, 4, 5), (PLAIN, 3), (OVER, 14), (SETTLE, 2), (SPLIT, 2), (MUL, 2, 0, 2),
    (BACK, 2, 0, 2), (OVER, 15), (RELAY, 3, 0, 2), (MUL, 2, 2, 3), (BACK, 2, 2, 3), (RELAY, 3, 2, 4),
    (CROSS, 3), (MUL, 0, 3, 4), (BACK, 0, 3, 4), (MUL, 1, 3, 4), (BACK, 1, 3, 4), (EARLY, 3),
    (MUL, 2, 3, 4), (BACK, 2, 3, 4), (HEAD, 3, 2, 4), (HEAD, 3, 0, 2), (SETTLE, 3), (SPLIT, 3),
    (MUL, 3, 2, 4), (BACK, 3, 2, 4), (MUL, 3, 0, 2), (BACK, 3, 0, 2), (ADD, 0, 0, 2), (ADD, 0, 2, 3),
    (ADD, 1, 0, 2), (ADD, 1, 2, 3), (ADD, 2, 0, 2), (ADD, 2, 2, 3), (ADD, 0, 3, 4), (ADD, 1, 3, 4),
    (ADD, 2, 3, 4), (ADD, 3, 2, 4), (ADD, 3, 0, 2), (FINISH, 0), (FINISH, 1), (FINISH, 2), (FINISH, 3),
    (DRAIN,),
)


def bulk_wait(ref, sem):
    pltpu.make_async_copy(ref, ref, sem).wait()


def kernel(
    left_ref, right_ref, out_ref,
    lbuf, s1, ag, braw, bs, asp, cp, cr, fin, outs, head,
    l_own, a1_send, a1_recv, a2_send, z_recv, relay_recv, plain_recv, far_recv, a3_send,
    b_send, b_own, b_par, b_oth, b_oc,
    c_send, c_recv, x_send, x_recv,
):
    G = GROUPS
    l = lax.axis_index("layer")
    z = lax.axis_index("row")
    q = lax.axis_index("col")
    c = q % 2
    h = (q // 2) % 2
    y = q // 4
    a = 2 * h + l
    rg = s1.shape[3]
    width = s1.shape[4]
    sub_rows = rg * G
    mine = a * 2 + c
    slot = h * 2 + c

    def col_of(yy, hh, cc):
        return yy * 4 + hh * 2 + cc

    def dev(dl=0, dz=0, dy=0, dh=0, dc=0):
        return ((l + dl) % 2, (z + dz) % 8, col_of((y + dy) % 4, (h + dh) % 2, (c + dc) % 2))

    def send(src, dst, send_sem, recv_sem, device):
        pltpu.make_async_remote_copy(
            src_ref=src, dst_ref=dst, send_sem=send_sem, recv_sem=recv_sem,
            device_id=device, device_id_type=MESH,
        ).start()

    partners = set()
    for dx in (0, 1):
        for dy in range(4):
            for dc in range(2):
                partners.add((dx, 0, dy, dx, dc))
    for dz in range(1, 8):
        partners.add((0, dz, 0, 0, 0))
    for dl in range(2):
        for dh in range(2):
            for dc in range(2):
                partners.add((dl, 0, 0, dh, dc))
    partners.discard((0, 0, 0, 0, 0))
    partners = sorted(partners)
    def split(x):
        high = x.astype(jnp.bfloat16)
        return high, (x - high.astype(jnp.float32)).astype(jnp.bfloat16)

    def split_right(which, start, size, block):
        rows = pl.ds(pl.multiple_of(start, size), size)
        tile = start // 256
        away = (tile % 4 - y + 4) % 4
        place = away + away // 2 - 2 * (away // 3)
        into = pl.ds(pl.multiple_of((place * 2 + tile // 4) * 256 + start % 256, size), size)
        cols = pl.ds(pl.multiple_of(block * 128, 128), 128)
        real = braw[which, 0, rows, :]
        imag = braw[which, 1, rows, :]
        for m, x in enumerate((real, imag, real + imag)):
            high, low = split(x)
            bs[m, 0, into, cols] = high
            bs[m, 1, into, cols] = low

    depth = braw.shape[2]

    def split_whole(which, block):
        @pl.loop(0, depth // 128)
        def _(i):
            split_right(which, i * 128, 128, block)

    with jax.named_scope("entry"):
        pltpu.make_async_copy(left_ref, lbuf, l_own).start()
        pltpu.make_async_copy(right_ref, braw.at[slot], b_own).start()
        barrier = pltpu.get_barrier_semaphore()
        for partner in partners:
            pl.semaphore_signal(barrier, inc=1, device_id=dev(*partner), device_id_type=MESH)
        pl.semaphore_wait(barrier, len(partners))
        bulk_wait(lbuf, l_own)

    def scatter(g):
        for dx in (1, 0):
            near_set = ((q // 2 - z + 6) % 8) // 4
            at = (2 * h + l) if dx == 0 else (2 * (1 - h) + (1 - l))
            for dy in (2, 1, 3, 0):
                for dc in (1, 0):
                    rows = (at * 2 + (c + dc) % 2) * sub_rows + g * rg
                    src_index = (
                        slice(None),
                        pl.ds(pl.multiple_of(rows, rg), rg),
                        pl.ds(pl.multiple_of(((y + dy) % 4) * width, width), width),
                    )
                    src = lbuf.at[src_index]
                    dst = s1.at[g, q]
                    if (dx, dy, dc) == (0, 0, 0):
                        pltpu.make_async_copy(
                            left_ref.at[src_index], dst, a1_recv.at[g, near_set]
                        ).start()
                    else:
                        send(src, dst, a1_send, a1_recv.at[g, near_set], dev(dx, 0, dy, dx, dc))

    def to_planes(g):
        for i, dz in enumerate(FAR_FIRST):
            if i % 4 == 0:
                bulk_wait(s1.at[g, pl.ds(0, 8)], a1_recv.at[g, i // 4])
            k = (z + dz) % 8
            send(
                s1.at[g, pl.ds(2 * k, 2)], ag.at[g, y, :, :, z], a2_send, z_recv.at[g, min(dz, 8 - dz) - 1], dev(0, dz)
            )
        ag[g, y, :, :, z] = s1[g, pl.ds(2 * z, 2)]

    def along_y(g, first, last):
        for j in range(first, last):
            if j:
                dz = ARRIVAL[ARRIVED[j][0]]
                bulk_wait(ag.at[g, y, :, :, pl.ds(0, len(ARRIVED[j]))], z_recv.at[g, min(dz, 8 - dz) - 1])
            for i in ARRIVED[j]:
                r = (z + ARRIVAL[i]) % 8
                piece = ag.at[g, y, :, :, r]
                src = piece if i else s1.at[g, pl.ds(2 * z, 2)]
                send(src, piece, a3_send, relay_recv.at[g, RELAY_OF[i]], dev(0, 0, 1 if i % 2 == 0 else 3))

    def plain(g):
        for i in range(8):
            piece = ag.at[g, y, :, :, (z + ARRIVAL[i]) % 8]
            src = piece if i else s1.at[g, pl.ds(2 * z, 2)]
            side = (i + 1) % 2
            send(src, piece, a3_send, plain_recv.at[g, side], dev(0, 0, (1, 3)[side]))

    def relay(g, first, last):
        for j in range(first, last):
            back, onward = (3, 1) if j % 2 == 0 else (1, 3)
            origin = (y + back) % 4
            bulk_wait(ag.at[g, origin, :, :, pl.ds(0, 2)], relay_recv.at[g, j])
            for i in RELAYED[j]:
                piece = ag.at[g, origin, :, :, (z + ARRIVAL[i]) % 8]
                send(piece, piece, a3_send, far_recv.at[g], dev(0, 0, onward))

    def near_in(g):
        for side in range(2):
            bulk_wait(ag.at[g, y, :, :, pl.ds(0, 4)], plain_recv.at[g, side])

    def settle(g):
        if g < G - 1:
            near_in(g)
        bulk_wait(ag.at[g, y], far_recv.at[g])

    half = depth // 2
    quarter = half // 2
    each = CHUNKS // 2
    chunk = quarter // each

    def start_of(which, core, i):
        return which * half + core * quarter + (i % each) * chunk

    def rows_of(which, core, i):
        return pl.ds(pl.multiple_of(start_of(which, core, i), chunk), chunk)

    def quarter_of(which, core):
        return pl.ds(pl.multiple_of(which * half + core * quarter, quarter), quarter)

    def near():
        bulk_wait(braw.at[slot], b_own)
        for which, core in ((1 - l, 1 - c), (1 - l, c), (l, 1 - c), (l, c)):
            piece = braw.at[slot, :, quarter_of(which, core)]
            send(piece, piece, b_send, b_par.at[which, core], dev(dc=1))

    near_other = h * 2 + 1 - c

    seen = []

    def first_quarter():
        if not seen:
            bulk_wait(braw.at[near_other, :, quarter_of(1 - l, c)], b_par.at[1 - l, c])
            seen.append(True)

    def far(i):
        first_quarter()
        piece = braw.at[h * 2 + i // each, :, rows_of(1 - l, c, i)]
        send(piece, piece, b_send, b_oth.at[0, i], dev(1, 0, 0, 1, 0))

    def partner():
        split_whole(slot, c)
        first_quarter()
        for which, core in ((1 - l, 1 - c), (l, c), (l, 1 - c)):
            bulk_wait(braw.at[near_other, :, quarter_of(which, core)], b_par.at[which, core])
        split_whole(near_other, 1 - c)

    def on(i):
        which = (1 - h) * 2 + i // each
        rows = rows_of(l, c, i)
        piece = braw.at[which, :, rows]
        bulk_wait(piece, b_oth.at[0, i])
        send(piece, piece, b_send, b_oth.at[1, i], dev(dl=1))
        send(piece, piece, b_send, b_oc.at[0, i // 4], dev(dc=1))
        split_right(which, start_of(l, c, i), chunk, 2 + i // each)

    def over(i):
        which = (1 - h) * 2 + i // each
        rows = rows_of(1 - l, c, i)
        piece = braw.at[which, :, rows]
        bulk_wait(piece, b_oth.at[1, i])
        send(piece, piece, b_send, b_oc.at[1, i // 4], dev(dc=1))
        split_right(which, start_of(1 - l, c, i), chunk, 2 + i // each)

    def cross(i):
        which = (1 - h) * 2 + 4 * i // each
        for k in range(2):
            start = (l if k == 0 else 1 - l) * half + (1 - c) * quarter + (4 * i % each) * chunk
            rows = pl.ds(pl.multiple_of(start, chunk), 4 * chunk)
            bulk_wait(braw.at[which, :, rows], b_oc.at[k, i])
            split_right(which, start, 4 * chunk, 2 + 4 * i // each)

    lines = 8 * rg

    def split_tiles(g, first, last):
        for t in range(first, last):
            for_k, from_y = t % 2, (y + SPREAD[t // 2]) % 4
            real = ag[g, from_y, for_k, 0].reshape(lines, width)
            imag = ag[g, from_y, for_k, 1].reshape(lines, width)
            for m, x in enumerate((real, imag, real + imag)):
                high, low = split(x)
                asp[g, m, :lines, t * width:(t + 1) * width] = high
                asp[g, m, lines:, t * width:(t + 1) * width] = low

    def split_left(g):
        split_tiles(g, 0 if g < G - 1 else 6, 8)

    def early(g):
        near_in(g)
        split_tiles(g, 0, 6)

    def dots(g, m, lo, hi, first, last):
        deep, cols = slice(first * width, last * width), slice(lo * 128, hi * 128)
        both = jnp.dot(asp[g, m, :, deep], bs[m, 0, deep, cols], preferred_element_type=jnp.float32)
        rest = jnp.dot(asp[g, m, :lines, deep], bs[m, 1, deep, cols], preferred_element_type=jnp.float32)
        return both[:lines] + both[lines:] + rest

    def begin(g, lo, hi):
        for m in range(3):
            head[m, :, lo * 128:hi * 128] = dots(g, m, lo, hi, 0, 6)

    def multiply(g, lo, hi):
        if g < G - 1:
            first, second, third = (dots(g, m, lo, hi, 0, 8) for m in range(3))
        else:
            first, second, third = (head[m, :, lo * 128:hi * 128] + dots(g, m, lo, hi, 6, 8) for m in range(3))
        for part, x in enumerate((first - second, third - first - second)):
            for b in range(lo, hi):
                cp[g, b, :, part] = x[:, (b - lo) * 128:(b - lo + 1) * 128].reshape(8, rg, 128)

    def hand_back(g, lo, hi):
        blocks = pl.ds(lo, hi - lo)
        for dz in FAR_FIRST:
            r = (z + dz) % 8
            send(cp.at[g, blocks, r], cr.at[g, blocks, z], c_send, c_recv.at[g, lo], dev(0, dz))

    def add_up(g, lo, hi):
        blocks = pl.ds(lo, hi - lo)
        bulk_wait(cr.at[g, blocks, pl.ds(0, 7)], c_recv.at[g, lo])
        total = cp[g, blocks, z]
        for dz in FAR_FIRST:
            total = total + cr[g, blocks, (z + dz) % 8]
        fin[g, lo:hi] = total
        for b in range(lo, hi):
            for dl in (1, 0):
                if b >= 2:
                    target = (l + dl) % 2, z, col_of(y, 1 - h, b - 2)
                    send(fin.at[g, b], outs.at[g, mine], x_send, x_recv.at[g], target)
                else:
                    dc = b
                    if dl or dc:
                        send(
                            fin.at[g, (c + dc) % 2], outs.at[g, mine], x_send, x_recv.at[g],
                            dev(dl, 0, 0, 0, dc),
                        )
        if lo == 0:
            outs[g, mine] = fin[g, c]

    def finish(g):
        bulk_wait(outs.at[g, pl.ds(0, 7)], x_recv.at[g])
        for i in range(8):
            out_ref[:, i * sub_rows + g * rg:i * sub_rows + (g + 1) * rg, :] = outs[g, i]

    def drain():
        bulk_wait(s1.at[:, pl.ds(0, 15)], a1_send)
        bulk_wait(s1.at[:, pl.ds(0, 14)], a2_send)
        bulk_wait(ag.at[:, pl.ds(0, 3)], a3_send)
        bulk_wait(cr.at[:, :, pl.ds(0, 7)], c_send)
        bulk_wait(outs.at[:, pl.ds(0, 7)], x_send)
        bulk_wait(braw.at[pl.ds(0, 3)], b_send)

    calls = (
        scatter, near, far, partner, to_planes, along_y, relay, on, over, cross,
        settle, split_left, multiply, hand_back, add_up, finish, drain, plain, early, begin,
    )
    for code, *numbers in ORDER:
        with jax.named_scope("_".join([calls[code].__name__, *map(str, numbers)])):
            calls[code](*numbers)


def local(left_matrix, right_matrix):
    _, rows, left_width = left_matrix.shape
    _, depth, cols = right_matrix.shape
    G = GROUPS
    rg = rows // 8 // G
    width = left_width // 4
    f32, bf16 = jnp.float32, jnp.bfloat16
    dma = pltpu.SemaphoreType.DMA
    return pl.pallas_call(
        kernel,
        out_shape=pltpu.VMEM((2, rows, cols), f32),
        in_specs=[pl.BlockSpec(memory_space=pl.ANY)] * 2,
        out_specs=pl.BlockSpec(memory_space=pltpu.VMEM),
        scratch_shapes=[
            pltpu.VMEM((2, rows, left_width), f32),
            pltpu.VMEM((G, 16, 2, rg, width), f32),
            pltpu.VMEM((G, 4, 2, 2, 8, rg, width), f32),
            pltpu.VMEM((4, 2, depth, cols), f32),
            pltpu.VMEM((3, 2, depth, 4 * cols), bf16),
            pltpu.VMEM((G, 3, 16 * rg, depth), bf16),
            pltpu.VMEM((G, 4, 8, 2, rg, cols), f32),
            pltpu.VMEM((G, 4, 8, 2, rg, cols), f32),
            pltpu.VMEM((G, 4, 2, rg, cols), f32),
            pltpu.VMEM((G, 8, 2, rg, cols), f32),
            pltpu.VMEM((3, 8 * rg, 4 * cols), f32),
            dma, dma, dma((G, 2)), dma, dma((G, 4)), dma((G, 4)), dma((G, 2)), dma((G,)), dma,
            dma, dma, dma((2, 2)), dma((2, CHUNKS)), dma((2, CHUNKS // 4)),
            dma, dma((G, 4)), dma, dma((G,)),
        ],
        compiler_params=pltpu.CompilerParams(
            collective_id=0, has_side_effects=True, vmem_limit_bytes=60 * 1024 * 1024
        ),
    )(left_matrix, right_matrix)


def solution(mesh):
    spec = P(None, "row", "col")
    return jax.shard_map(local, mesh=mesh, in_specs=(spec, spec), out_specs=spec, check_vma=False)
```

```python
import functools

import jax
import jax.numpy as jnp
from jax import lax
from jax.experimental import pallas as pl
from jax.experimental.pallas import tpu as pltpu
from jax.sharding import PartitionSpec as P

MESH = pl.DeviceIdType.MESH
GROUPS = 4
FAR_FIRST = (4, 3, 5, 2, 6, 1, 7)
ARRIVAL = (0, *FAR_FIRST)
ARRIVED = ((0,), (1,), (2, 3), (4, 5), (6, 7))
RELAYED = ((0, 2), (1, 3), (4, 6), (5, 7))
SPREAD = (0, 1, 3, 2)
RELAY_OF = {i: j for j, pair in enumerate(RELAYED) for i in pair}
CHUNKS = 16


SCATTER, NEAR, FAR, PARTNER, PLANES, Y, RELAY, ON, OVER, CROSS, SETTLE, SPLIT, MUL, BACK, ADD, FINISH, DRAIN, PLAIN, EARLY, HEAD = range(20)
PARTS = (((0, 2), (2, 3), (3, 4)), ((0, 2), (2, 3), (3, 4)), ((0, 2), (2, 3), (3, 4)), ((0, 2), (2, 4)))
ORDER = (
    (SCATTER, 0), (NEAR,), (SCATTER, 1), (SCATTER, 2), (PARTNER,), (PLANES, 0), (Y, 0, 0, 1), (FAR, 0),
    (SCATTER, 3), (PLANES, 1), (Y, 1, 0, 1), (FAR, 1), (Y, 0, 1, 2), (PLANES, 2), (Y, 2, 0, 1), (FAR, 2),
    (Y, 0, 2, 3), (ON, 0), (Y, 0, 3, 4), (FAR, 3), (Y, 0, 4, 5), (PLAIN, 0), (FAR, 4), (PLANES, 3),
    (OVER, 0), (FAR, 5), (ON, 1), (RELAY, 0, 0, 2), (Y, 1, 1, 2), (FAR, 6), (Y, 1, 2, 3), (ON, 2),
    (RELAY, 0, 2, 4), (Y, 1, 3, 4), (FAR, 7), (ON, 3), (Y, 1, 4, 5), (OVER, 1), (FAR, 8), (ON, 4),
    (OVER, 2), (FAR, 9), (PLAIN, 1), (ON, 5), (RELAY, 1, 0, 2), (OVER, 3), (FAR, 10), (ON, 6),
    (SETTLE, 0), (SPLIT, 0), (OVER, 4), (FAR, 11), (ON, 7), (MUL, 0, 0, 2), (FAR, 12), (BACK, 0, 0, 2),
    (ON, 8), (OVER, 5), (RELAY, 1, 2, 4), (CROSS, 0), (Y, 2, 1, 3), (OVER, 6), (FAR, 13), (ON, 9),
    (Y, 2, 3, 5), (OVER, 7), (FAR, 14), (ON, 10), (PLAIN, 2), (OVER, 8), (FAR, 15), (ON, 11),
    (SETTLE, 1), (CROSS, 1), (OVER, 9), (SPLIT, 1), (ON, 12), (RELAY, 2, 0, 2), (MUL, 0, 2, 3),
    (BACK, 0, 2, 3), (OVER, 10), (ON, 13), (RELAY, 2, 2, 4), (MUL, 1, 0, 2), (BACK, 1, 0, 2), (ON, 14),
    (OVER, 11), (MUL, 1, 2, 3), (BACK, 1, 2, 3), (OVER, 12), (Y, 3, 0, 1), (ON, 15), (Y, 3, 1, 3),
    (OVER, 13), (Y, 3, 3, 4), (CROSS, 2), (Y, 3, 4, 5), (PLAIN, 3), (OVER, 14), (SETTLE, 2), (SPLIT, 2),
    (MUL, 2, 0, 2), (BACK, 2, 0, 2), (OVER, 15), (RELAY, 3, 0, 2), (MUL, 2, 2, 3), (BACK, 2, 2, 3),
    (RELAY, 3, 2, 4), (CROSS, 3), (MUL, 0, 3, 4), (BACK, 0, 3, 4), (MUL, 1, 3, 4), (BACK, 1, 3, 4),
    (EARLY, 3), (MUL, 2, 3, 4), (BACK, 2, 3, 4), (HEAD, 3, 2, 4), (SETTLE, 3), (SPLIT, 3),
    (MUL, 3, 2, 4), (BACK, 3, 2, 4), (HEAD, 3, 0, 2), (MUL, 3, 0, 2), (BACK, 3, 0, 2), (ADD, 0, 0, 2),
    (ADD, 0, 2, 3), (ADD, 1, 0, 2), (ADD, 1, 2, 3), (ADD, 2, 0, 2), (ADD, 2, 2, 3), (ADD, 0, 3, 4),
    (ADD, 1, 3, 4), (ADD, 2, 3, 4), (ADD, 3, 2, 4), (ADD, 3, 0, 2), (FINISH, 0), (FINISH, 1),
    (FINISH, 2), (FINISH, 3), (DRAIN,),
)


def bulk_wait(ref, sem):
    pltpu.make_async_copy(ref, ref, sem).wait()


def kernel(
    left_ref, right_ref, out_ref,
    lbuf, s1, ag, braw, bs, asp, cp, cr, fin, outs, head,
    l_own, a1_send, a1_recv, a2_send, z_recv, relay_recv, plain_recv, far_recv, a3_send,
    b_send, b_own, b_par, b_oth, b_oc,
    c_send, c_recv, x_send, x_recv,
):
    G = GROUPS
    l = lax.axis_index("layer")
    z = lax.axis_index("row")
    q = lax.axis_index("col")
    c = q % 2
    h = (q // 2) % 2
    y = q // 4
    a = 2 * h + l
    rg = s1.shape[3]
    width = s1.shape[4]
    sub_rows = rg * G
    mine = a * 2 + c
    slot = h * 2 + c

    def col_of(yy, hh, cc):
        return yy * 4 + hh * 2 + cc

    def dev(dl=0, dz=0, dy=0, dh=0, dc=0):
        return ((l + dl) % 2, (z + dz) % 8, col_of((y + dy) % 4, (h + dh) % 2, (c + dc) % 2))

    def send(src, dst, send_sem, recv_sem, device):
        pltpu.make_async_remote_copy(
            src_ref=src, dst_ref=dst, send_sem=send_sem, recv_sem=recv_sem,
            device_id=device, device_id_type=MESH,
        ).start()

    partners = set()
    for dx in (0, 1):
        for dy in range(4):
            for dc in range(2):
                partners.add((dx, 0, dy, dx, dc))
    for dz in range(1, 8):
        partners.add((0, dz, 0, 0, 0))
    for dl in range(2):
        for dh in range(2):
            for dc in range(2):
                partners.add((dl, 0, 0, dh, dc))
    partners.discard((0, 0, 0, 0, 0))
    partners = sorted(partners)
    def split(x):
        high = x.astype(jnp.bfloat16)
        return high, (x - high.astype(jnp.float32)).astype(jnp.bfloat16)

    def split_right(which, start, size, block):
        rows = pl.ds(pl.multiple_of(start, size), size)
        tile = start // 256
        away = (tile % 4 - y + 4) % 4
        place = away + away // 2 - 2 * (away // 3)
        into = pl.ds(pl.multiple_of((place * 2 + tile // 4) * 256 + start % 256, size), size)
        cols = pl.ds(pl.multiple_of(block * 128, 128), 128)
        real = braw[which, 0, rows, :]
        imag = braw[which, 1, rows, :]
        for m, x in enumerate((real, imag, real + imag)):
            high, low = split(x)
            bs[m, 0, into, cols] = high
            bs[m, 1, into, cols] = low

    depth = braw.shape[2]

    def split_whole(which, block):
        @pl.loop(0, depth // 128)
        def _(i):
            split_right(which, i * 128, 128, block)

    with jax.named_scope("entry"):
        pltpu.make_async_copy(left_ref, lbuf, l_own).start()
        pltpu.make_async_copy(right_ref, braw.at[slot], b_own).start()
        barrier = pltpu.get_barrier_semaphore()
        for partner in partners:
            pl.semaphore_signal(barrier, inc=1, device_id=dev(*partner), device_id_type=MESH)
        pl.semaphore_wait(barrier, len(partners))
        bulk_wait(lbuf, l_own)

    def scatter(g):
        for dx in (1, 0):
            near_set = ((q // 2 - z + 6) % 8) // 4
            at = (2 * h + l) if dx == 0 else (2 * (1 - h) + (1 - l))
            for dy in (2, 1, 3, 0):
                for dc in (1, 0):
                    rows = (at * 2 + (c + dc) % 2) * sub_rows + g * rg
                    src_index = (
                        slice(None),
                        pl.ds(pl.multiple_of(rows, rg), rg),
                        pl.ds(pl.multiple_of(((y + dy) % 4) * width, width), width),
                    )
                    src = lbuf.at[src_index]
                    dst = s1.at[g, q]
                    if (dx, dy, dc) == (0, 0, 0):
                        pltpu.make_async_copy(
                            left_ref.at[src_index], dst, a1_recv.at[g, near_set]
                        ).start()
                    else:
                        send(src, dst, a1_send, a1_recv.at[g, near_set], dev(dx, 0, dy, dx, dc))

    def to_planes(g):
        for i, dz in enumerate(FAR_FIRST):
            if i % 4 == 0:
                bulk_wait(s1.at[g, pl.ds(0, 8)], a1_recv.at[g, i // 4])
            k = (z + dz) % 8
            send(
                s1.at[g, pl.ds(2 * k, 2)], ag.at[g, y, :, :, z], a2_send, z_recv.at[g, min(dz, 8 - dz) - 1], dev(0, dz)
            )
        ag[g, y, :, :, z] = s1[g, pl.ds(2 * z, 2)]

    def along_y(g, first, last):
        for j in range(first, last):
            if j:
                dz = ARRIVAL[ARRIVED[j][0]]
                bulk_wait(ag.at[g, y, :, :, pl.ds(0, len(ARRIVED[j]))], z_recv.at[g, min(dz, 8 - dz) - 1])
            for i in ARRIVED[j]:
                r = (z + ARRIVAL[i]) % 8
                piece = ag.at[g, y, :, :, r]
                src = piece if i else s1.at[g, pl.ds(2 * z, 2)]
                send(src, piece, a3_send, relay_recv.at[g, RELAY_OF[i]], dev(0, 0, 1 if i % 2 == 0 else 3))

    def plain(g):
        for i in range(8):
            piece = ag.at[g, y, :, :, (z + ARRIVAL[i]) % 8]
            src = piece if i else s1.at[g, pl.ds(2 * z, 2)]
            side = (i + 1) % 2
            send(src, piece, a3_send, plain_recv.at[g, side], dev(0, 0, (1, 3)[side]))

    def relay(g, first, last):
        for j in range(first, last):
            back, onward = (3, 1) if j % 2 == 0 else (1, 3)
            origin = (y + back) % 4
            bulk_wait(ag.at[g, origin, :, :, pl.ds(0, 2)], relay_recv.at[g, j])
            for i in RELAYED[j]:
                piece = ag.at[g, origin, :, :, (z + ARRIVAL[i]) % 8]
                send(piece, piece, a3_send, far_recv.at[g], dev(0, 0, onward))

    def near_in(g):
        for side in range(2):
            bulk_wait(ag.at[g, y, :, :, pl.ds(0, 4)], plain_recv.at[g, side])

    def settle(g):
        if g < G - 1:
            near_in(g)
        bulk_wait(ag.at[g, y], far_recv.at[g])

    half = depth // 2
    quarter = half // 2
    each = CHUNKS // 2
    chunk = quarter // each

    def start_of(which, core, i):
        return which * half + core * quarter + (i % each) * chunk

    def rows_of(which, core, i):
        return pl.ds(pl.multiple_of(start_of(which, core, i), chunk), chunk)

    def quarter_of(which, core):
        return pl.ds(pl.multiple_of(which * half + core * quarter, quarter), quarter)

    def near():
        bulk_wait(braw.at[slot], b_own)
        for which, core in ((1 - l, 1 - c), (1 - l, c), (l, 1 - c), (l, c)):
            piece = braw.at[slot, :, quarter_of(which, core)]
            send(piece, piece, b_send, b_par.at[which, core], dev(dc=1))

    near_other = h * 2 + 1 - c

    seen = []

    def first_quarter():
        if not seen:
            bulk_wait(braw.at[near_other, :, quarter_of(1 - l, c)], b_par.at[1 - l, c])
            seen.append(True)

    def far(i):
        first_quarter()
        piece = braw.at[h * 2 + i // each, :, rows_of(1 - l, c, i)]
        send(piece, piece, b_send, b_oth.at[0, i], dev(1, 0, 0, 1, 0))

    def partner():
        split_whole(slot, c)
        first_quarter()
        for which, core in ((1 - l, 1 - c), (l, c), (l, 1 - c)):
            bulk_wait(braw.at[near_other, :, quarter_of(which, core)], b_par.at[which, core])
        split_whole(near_other, 1 - c)

    def on(i):
        which = (1 - h) * 2 + i // each
        rows = rows_of(l, c, i)
        piece = braw.at[which, :, rows]
        bulk_wait(piece, b_oth.at[0, i])
        send(piece, piece, b_send, b_oth.at[1, i], dev(dl=1))
        send(piece, piece, b_send, b_oc.at[0, i // 4], dev(dc=1))
        split_right(which, start_of(l, c, i), chunk, 2 + i // each)

    def over(i):
        which = (1 - h) * 2 + i // each
        rows = rows_of(1 - l, c, i)
        piece = braw.at[which, :, rows]
        bulk_wait(piece, b_oth.at[1, i])
        send(piece, piece, b_send, b_oc.at[1, i // 4], dev(dc=1))
        split_right(which, start_of(1 - l, c, i), chunk, 2 + i // each)

    def cross(i):
        which = (1 - h) * 2 + 4 * i // each
        for k in range(2):
            start = (l if k == 0 else 1 - l) * half + (1 - c) * quarter + (4 * i % each) * chunk
            rows = pl.ds(pl.multiple_of(start, chunk), 4 * chunk)
            bulk_wait(braw.at[which, :, rows], b_oc.at[k, i])
            split_right(which, start, 4 * chunk, 2 + 4 * i // each)

    lines = 8 * rg

    def split_tiles(g, first, last):
        for t in range(first, last):
            for_k, from_y = t % 2, (y + SPREAD[t // 2]) % 4
            real = ag[g, from_y, for_k, 0].reshape(lines, width)
            imag = ag[g, from_y, for_k, 1].reshape(lines, width)
            for m, x in enumerate((real, imag, real + imag)):
                high, low = split(x)
                asp[g, m, :lines, t * width:(t + 1) * width] = high
                asp[g, m, lines:, t * width:(t + 1) * width] = low

    def split_left(g):
        split_tiles(g, 0 if g < G - 1 else 6, 8)

    def early(g):
        near_in(g)
        split_tiles(g, 0, 6)

    def dots(g, m, lo, hi, first, last):
        deep, cols = slice(first * width, last * width), slice(lo * 128, hi * 128)
        both = jnp.dot(asp[g, m, :, deep], bs[m, 0, deep, cols], preferred_element_type=jnp.float32)
        rest = jnp.dot(asp[g, m, :lines, deep], bs[m, 1, deep, cols], preferred_element_type=jnp.float32)
        return both[:lines] + both[lines:] + rest

    def begin(g, lo, hi):
        for m in range(3):
            head[m, :, lo * 128:hi * 128] = dots(g, m, lo, hi, 0, 6)

    def multiply(g, lo, hi):
        if g < G - 1:
            first, second, third = (dots(g, m, lo, hi, 0, 8) for m in range(3))
        else:
            first, second, third = (head[m, :, lo * 128:hi * 128] + dots(g, m, lo, hi, 6, 8) for m in range(3))
        for part, x in enumerate((first - second, third - first - second)):
            for b in range(lo, hi):
                cp[g, b, :, part] = x[:, (b - lo) * 128:(b - lo + 1) * 128].reshape(8, rg, 128)

    def hand_back(g, lo, hi):
        blocks = pl.ds(lo, hi - lo)
        for dz in FAR_FIRST:
            r = (z + dz) % 8
            send(cp.at[g, blocks, r], cr.at[g, blocks, z], c_send, c_recv.at[g, lo], dev(0, dz))

    def add_up(g, lo, hi):
        blocks = pl.ds(lo, hi - lo)
        bulk_wait(cr.at[g, blocks, pl.ds(0, 7)], c_recv.at[g, lo])
        total = cp[g, blocks, z]
        for dz in FAR_FIRST:
            total = total + cr[g, blocks, (z + dz) % 8]
        fin[g, lo:hi] = total
        for b in range(lo, hi):
            for dl in (1, 0):
                if b >= 2:
                    target = (l + dl) % 2, z, col_of(y, 1 - h, b - 2)
                    send(fin.at[g, b], outs.at[g, mine], x_send, x_recv.at[g], target)
                else:
                    dc = b
                    if dl or dc:
                        send(
                            fin.at[g, (c + dc) % 2], outs.at[g, mine], x_send, x_recv.at[g],
                            dev(dl, 0, 0, 0, dc),
                        )
        if lo == 0:
            outs[g, mine] = fin[g, c]

    def finish(g):
        bulk_wait(outs.at[g, pl.ds(0, 7)], x_recv.at[g])
        for i in range(8):
            out_ref[:, i * sub_rows + g * rg:i * sub_rows + (g + 1) * rg, :] = outs[g, i]

    def drain():
        bulk_wait(s1.at[:, pl.ds(0, 15)], a1_send)
        bulk_wait(s1.at[:, pl.ds(0, 14)], a2_send)
        bulk_wait(ag.at[:, pl.ds(0, 3)], a3_send)
        bulk_wait(cr.at[:, :, pl.ds(0, 7)], c_send)
        bulk_wait(outs.at[:, pl.ds(0, 7)], x_send)
        bulk_wait(braw.at[pl.ds(0, 3)], b_send)

    calls = (
        scatter, near, far, partner, to_planes, along_y, relay, on, over, cross,
        settle, split_left, multiply, hand_back, add_up, finish, drain, plain, early, begin,
    )
    for code, *numbers in ORDER:
        with jax.named_scope("_".join([calls[code].__name__, *map(str, numbers)])):
            calls[code](*numbers)


def local(left_matrix, right_matrix):
    _, rows, left_width = left_matrix.shape
    _, depth, cols = right_matrix.shape
    G = GROUPS
    rg = rows // 8 // G
    width = left_width // 4
    f32, bf16 = jnp.float32, jnp.bfloat16
    dma = pltpu.SemaphoreType.DMA
    return pl.pallas_call(
        kernel,
        out_shape=pltpu.VMEM((2, rows, cols), f32),
        in_specs=[pl.BlockSpec(memory_space=pl.ANY)] * 2,
        out_specs=pl.BlockSpec(memory_space=pltpu.VMEM),
        scratch_shapes=[
            pltpu.VMEM((2, rows, left_width), f32),
            pltpu.VMEM((G, 16, 2, rg, width), f32),
            pltpu.VMEM((G, 4, 2, 2, 8, rg, width), f32),
            pltpu.VMEM((4, 2, depth, cols), f32),
            pltpu.VMEM((3, 2, depth, 4 * cols), bf16),
            pltpu.VMEM((G, 3, 16 * rg, depth), bf16),
            pltpu.VMEM((G, 4, 8, 2, rg, cols), f32),
            pltpu.VMEM((G, 4, 8, 2, rg, cols), f32),
            pltpu.VMEM((G, 4, 2, rg, cols), f32),
            pltpu.VMEM((G, 8, 2, rg, cols), f32),
            pltpu.VMEM((3, 8 * rg, 4 * cols), f32),
            dma, dma, dma((G, 2)), dma, dma((G, 4)), dma((G, 4)), dma((G, 2)), dma((G,)), dma,
            dma, dma, dma((2, 2)), dma((2, CHUNKS)), dma((2, CHUNKS // 4)),
            dma, dma((G, 4)), dma, dma((G,)),
        ],
        compiler_params=pltpu.CompilerParams(
            collective_id=0, has_side_effects=True, vmem_limit_bytes=60 * 1024 * 1024
        ),
    )(left_matrix, right_matrix)


def solution(mesh):
    spec = P(None, "row", "col")
    return jax.shard_map(local, mesh=mesh, in_specs=(spec, spec), out_specs=spec, check_vma=False)
```
